8 devices in a mesh: dp: 1 (over z), sp: 8 (over x, y, core).
Axes of the slice: x: 2, y: 2, z: 1, core: 2. Of those that a mesh axis runs over, the one named last changes fastest.
Arguments:
- x: bfloat16 [4096, 8192], P(('dp', 'sp'))
- gain: bfloat16 [8192], replicated
- wq: bfloat16 [8192, 8192], P('sp')
- wk: bfloat16 [8192, 256], P('sp')
- wv: bfloat16 [8192, 256], P('sp')
- wo: bfloat16 [8192, 8192], P('sp')
Outputs:
- output: bfloat16 [4096, 8192], P(('dp', 'sp'))
All inputs are finite; a program needn't handle non-finite values.
Results may differ from the reference program's by a relative error of at most 0.012.
Values are sent between devices in bfloat16 or wider.
A program may use at most 2 GiB of HBM per device.

```python
import jax
import jax.numpy as jnp
from jax import lax

ROWS = 4096
D = 8192
HEADS = 32
KV_HEADS = 1
HEAD = 256
THETA = 10000


def setup_inputs(seed: int = 0, part: int = 0) -> dict:
    kx, kn, kq, kk, kv, ko = jax.random.split(jax.random.key(seed), 6)

    def weights(key, rows, columns):
        return jax.random.normal(key, (rows, columns), jnp.float32) * rows**-0.5

    drawn = {
        "x": jax.random.normal(jax.random.fold_in(kx, part), (ROWS, D), jnp.float32),
        "gain": 1 + 0.1 * jax.random.normal(kn, (D,), jnp.float32),
        "wq": 2 * weights(kq, D, HEADS * HEAD),
        "wk": 2 * weights(kk, D, KV_HEADS * HEAD),
        "wv": 4 * weights(kv, D, KV_HEADS * HEAD),
        "wo": weights(ko, HEADS * HEAD, D),
    }
    return {k: v.astype(jnp.bfloat16) for k, v in drawn.items()}


def normed(x, gain):
    wide = x.astype(jnp.float32)
    scale = lax.rsqrt(jnp.mean(wide * wide, -1, keepdims=True) + 1e-6)
    return (wide * scale * gain.astype(jnp.float32)).astype(jnp.bfloat16)


def turned(t, place, theta):
    half = t.shape[-1] // 2
    angle = place.astype(jnp.float32)[:, None] * theta ** (-jnp.arange(half, dtype=jnp.float32) / half)
    cos, sin = jnp.cos(angle)[:, None], jnp.sin(angle)[:, None]
    a, b = t[..., :half].astype(jnp.float32), t[..., half:].astype(jnp.float32)
    return jnp.concatenate([a * cos - b * sin, b * cos + a * sin], -1).astype(jnp.bfloat16)


def matmul(a, w):
    return jnp.dot(a, w, preferred_element_type=jnp.float32).astype(jnp.bfloat16)


def einsum(form, a, b):
    return jnp.einsum(form, a.astype(jnp.float32), b.astype(jnp.float32))


def attention(q, k, v):
    scores = einsum("tgsd,ugd->gstu", q, k) * q.shape[-1] ** -0.5
    token = jnp.arange(q.shape[0])
    scores = jnp.where(token[:, None] >= token, scores, -jnp.inf)
    weights = jax.nn.softmax(scores, -1).astype(jnp.bfloat16)
    return einsum("gstu,ugd->tgsd", weights, v).astype(jnp.bfloat16)


def reference(x, gain, wq, wk, wv, wo):
    a, place = normed(x, gain), jnp.arange(ROWS)
    q = turned(matmul(a, wq).reshape(ROWS, HEADS, HEAD), place, THETA).reshape(ROWS, KV_HEADS, -1, HEAD)
    k = turned(matmul(a, wk).reshape(ROWS, KV_HEADS, HEAD), place, THETA)
    v = matmul(a, wv).reshape(ROWS, KV_HEADS, HEAD)
    seen = attention(q, k, v).reshape(ROWS, HEADS * HEAD)
    return (x.astype(jnp.float32) + jnp.dot(seen, wo, preferred_element_type=jnp.float32)).astype(jnp.bfloat16)
```

```python
import functools

import jax
import jax.numpy as jnp
from jax import lax
from jax.experimental import pallas as pl
from jax.experimental.pallas import tpu as pltpu
from jax.sharding import PartitionSpec as P

HEAD = 256
THETA = 10000
NEG = -1e30
HIDDEN = 2 * NEG
LOG2E = 1.4426950408889634
MESH = pl.DeviceIdType.MESH
D = 8192
OWN = 512
TOK = 2 * OWN
ROWS = 1024
HEADS = 16
G = HEADS + 1
CW = 256
NC = D // CW
PIECE = 128
STRIP = 512
VMEM = 63 * 2**20


def _dot(a, b, ca=1, cb=0):
    return lax.dot_general(a, b, (((ca,), (cb,)), ((), ())), preferred_element_type=jnp.float32)


def _turn(t, cos, sin):
    a, b = t[:, : HEAD // 2], t[:, HEAD // 2 :]
    return jnp.concatenate([a * cos - b * sin, b * cos + a * sin], axis=-1).astype(jnp.bfloat16)


def _kernel(x, gain, wkv, wq, wo, cos, sin, y, WQ, WO, PR,
            A, KV, VT, seen, wbuf, q_s, acc, top_s, mix_s, wob, pbuf, obuf, prb, xb, yb,
            sy, ry, sx, rx, sf, rf, sd, rd, sxp, rxp, lxp, sk, rk, wst, swx, rwx, swd, rwd, wos, sp, rp, prs, xcs, ys):
    me = lax.axis_index("sp")
    i, j, c = lax.div(me, 4), lax.rem(lax.div(me, 2), 2), lax.rem(me, 2)
    sib, yn, xn = me + 1 - 2 * c, me + 2 - 4 * j, me + 4 - 8 * i

    def remote(src, dst, s, r, dev):
        return pltpu.make_async_remote_copy(src_ref=src, dst_ref=dst, send_sem=s, recv_sem=r, device_id={"sp": dev}, device_id_type=MESH)

    def rows(e):
        return pl.ds(pl.multiple_of(e * ROWS, ROWS), ROWS)

    def qcols(jj, g):
        h = g - 1
        return pl.ds(pl.multiple_of(lax.div(h, 8) * 4096 + jj * 2048 + lax.rem(h, 8) * HEAD, HEAD), HEAD)

    def kvcols(jj):
        return pl.ds(pl.multiple_of(jj * HEAD, HEAD), HEAD)

    def mate(b):
        b2, b1, b0 = lax.div(b, 4), lax.rem(lax.div(b, 2), 2), lax.rem(b, 2)
        return 4 * lax.rem(i + b1, 2) + 2 * lax.rem(j + b2, 2) + lax.rem(c + b0, 2)

    def own_y(g):
        return remote(wq.at[:, qcols(1 - j, g)], WQ.at[g, rows(me), :], sy.at[g], ry.at[g], yn)

    def own_x(g):
        return remote(wq.at[:, qcols(j, g)], WQ.at[g, rows(me), :], sx.at[g], rx.at[g], xn)

    def own_d(g):
        return remote(wq.at[:, qcols(j, g)], WQ.at[g, rows(me), :], sd.at[g, 0], rd.at[g, 0], sib)

    def pass_x(g):
        return remote(WQ.at[g, rows(yn), :], WQ.at[g, rows(yn), :], sf.at[g], rf.at[g], xn)

    def pass_d(g, kind):
        e = {1: yn, 2: xn, 3: xn + yn - me}[kind]
        return remote(WQ.at[g, rows(e), :], WQ.at[g, rows(e), :], sd.at[g, kind], rd.at[g, kind], sib)

    def got_y(g):
        remote(WQ.at[g, rows(yn), :], WQ.at[g, rows(yn), :], sy.at[g], ry.at[g], yn).wait_recv()

    def got_x(g):
        remote(WQ.at[g, rows(xn), :], WQ.at[g, rows(xn), :], sx.at[g], rx.at[g], xn).wait_recv()

    def got_f(g):
        e = xn + yn - me
        remote(WQ.at[g, rows(e), :], WQ.at[g, rows(e), :], sf.at[g], rf.at[g], xn).wait_recv()

    def got_d(g, kind):
        e = {0: sib, 1: yn + sib - me, 2: xn + sib - me, 3: xn + yn + sib - 2 * me}[kind]
        remote(WQ.at[g, rows(e), :], WQ.at[g, rows(e), :], sd.at[g, kind], rd.at[g, kind], sib).wait_recv()

    def stage(g, b):
        e = mate(b)
        return pltpu.make_async_copy(WQ.at[g, rows(e), :], wbuf.at[lax.rem(g, 2), rows(e), :], wst.at[lax.rem(g, 2), b])

    def stage_own(g):
        return pltpu.make_async_copy(wq.at[:, qcols(j, g)], wbuf.at[lax.rem(g, 2), rows(me), :], wst.at[lax.rem(g, 2), 0])

    def stage_early(g):
        stage_own(g).start()
        got_d(g, 0)
        stage(g, 1).start()
        stage(g, 2).start()
        got_d(g, 2)
        stage(g, 3).start()
        stage(g, 4).start()
        got_d(g, 1)
        stage(g, 5).start()

    def wo_x(n):
        cols = pl.ds(pl.multiple_of(n * CW, CW), CW)
        return remote(wo.at[:, cols], WO.at[n, rows(2 * i + c), :], swx.at[n], rwx.at[n], xn)

    def wo_d(n):
        cols = pl.ds(pl.multiple_of(n * CW, CW), CW)
        return remote(wo.at[:, cols], WO.at[n, rows(2 * i + c), :], swd.at[n, 0], rwd.at[n, 0], sib)

    def wo_pass(n):
        r = rows(2 * (1 - i) + c)
        return remote(WO.at[n, r, :], WO.at[n, r, :], swd.at[n, 1], rwd.at[n, 1], sib)

    def kv_block(kv, cc, ij, s, dev):
        return remote(KV.at[kv, cc, ij], KV.at[kv, cc, ij], s, rk.at[kv, cc, ij], dev)

    barrier = pltpu.get_barrier_semaphore()
    for dev in (sib, yn, xn):
        pl.semaphore_signal(barrier, inc=1, device_id={"sp": dev}, device_id_type=MESH)
    pl.semaphore_wait(barrier, 3)

    remote(wkv.at[:, kvcols(1 - j)], WQ.at[0, rows(me), :], sy.at[0], ry.at[0], yn).start()
    remote(wkv.at[:, kvcols(j)], WQ.at[0, rows(me), :], sx.at[0], rx.at[0], xn).start()
    remote(wkv.at[:, kvcols(j)], WQ.at[0, rows(me), :], sd.at[0, 0], rd.at[0, 0], sib).start()

    def x_piece(p, jj, dev):
        return remote(x.at[pl.ds(p * PIECE, PIECE), :], A.at[pl.ds(pl.multiple_of(jj * OWN + p * PIECE, PIECE), PIECE), :], sxp.at[p], rxp.at[p], dev)

    def x_local(p):
        return pltpu.make_async_copy(x.at[pl.ds(p * PIECE, PIECE), :], A.at[pl.ds(pl.multiple_of(j * OWN + p * PIECE, PIECE), PIECE), :], lxp.at[p])

    pieces = OWN // PIECE
    for p in range(pieces):
        x_piece(p, j, yn).start()
        x_local(p).start()
    own_x(1).start()
    own_x(2).start()

    @pl.loop(1, G)
    def _(g):
        own_d(g).start()

    pltpu.make_async_copy(wkv.at[:, kvcols(j)], wbuf.at[0, rows(me), :], wst.at[0, 0]).start()
    got_y(0)
    pass_x(0).start()
    pass_d(0, 1).start()
    stage(0, 4).start()

    @pl.loop(3, G)
    def _(g):
        own_x(g).start()

    got_x(0)
    pass_d(0, 2).start()
    stage(0, 2).start()
    got_f(0)
    pass_d(0, 3).start()
    stage(0, 6).start()
    for kind, b in ((0, 1), (2, 3), (1, 5), (3, 7)):
        got_d(0, kind)
        stage(0, b).start()
    for b in range(8):
        stage(0, b).wait()

    def norm_and_kv(p, jj):
        at = pl.multiple_of(jj * OWN + p * PIECE, PIECE)

        @pl.loop(0, PIECE // 16)
        def _(r):
            here = pl.ds(pl.multiple_of(at + r * 16, 16), 16)
            wide = A[here, :].astype(jnp.float32)
            scale = lax.rsqrt(jnp.mean(wide * wide, -1, keepdims=True) + 1e-6)
            A[here, :] = (wide * scale * gain[...].astype(jnp.float32)).astype(jnp.bfloat16)

        here = pl.ds(at, PIECE)
        t = _dot(A[here, :], wbuf[0]).astype(jnp.bfloat16)
        turned = _turn(t.astype(jnp.float32), cos[here, :], sin[here, :])
        KV[j, c, 2 * i + jj, pl.ds(pl.multiple_of(p * PIECE, PIECE), PIECE), :] = jnp.where(j == 0, turned, t)

    def kv_send(jj, which):
        for k, dev in enumerate((yn, xn, sib)):
            kv_block(j, c, 2 * i + jj, sk.at[k, which], dev).start()

    @pl.loop(0, pieces)
    def _(p):
        x_local(p).wait()
        norm_and_kv(p, j)

    kv_send(j, 0)

    @pl.loop(0, pieces)
    def _(p):
        for n in range(3):
            g = 3 * p + n + 1
            got_x(g)
            pass_d(g, 2).start()
        x_piece(p, 1 - j, yn).wait_recv()
        norm_and_kv(p, 1 - j)

    kv_send(1 - j, 1)

    for which, jj in enumerate((j, 1 - j)):
        kv_block(j, c, 2 * (1 - i) + jj, sk.at[3, which], xn).wait_recv()
        kv_block(j, c, 2 * (1 - i) + jj, sk.at[3, which], yn).start()
        kv_block(j, c, 2 * (1 - i) + jj, sk.at[4, which], sib).start()
    own_y(1).start()
    own_y(2).start()
    own_y(3).start()

    @pl.loop(3 * pieces + 1, G)
    def _(g):
        got_x(g)
        pass_d(g, 2).start()

    for which, ij in enumerate((2 * i, 2 * i + 1)):
        kv_block(1 - j, c, ij, sk.at[5, which], yn).wait_recv()
        kv_block(1 - j, c, ij, sk.at[5, which], sib).start()
    for which, ij in enumerate((2 * (1 - i), 2 * (1 - i) + 1)):
        kv_block(1 - j, c, ij, sk.at[6, which], yn).wait_recv()
        kv_block(1 - j, c, ij, sk.at[6, which], sib).start()
    for kv in range(2):
        for ij in range(4):
            kv_block(kv, 1 - c, ij, sk.at[6, 0], sib).wait_recv()

    @pl.loop(0, 8)
    def _(t):
        VT[t, :HEAD, :] = KV[1, lax.rem(t, 2), lax.div(t, 2)].T
        VT[t, HEAD:, :] = jnp.ones((8, OWN), jnp.bfloat16)

    e2 = HEAD**-0.5 * LOG2E
    low = 4 * i + c

    def block(t, strips):
        k, vt = KV[0, lax.rem(t, 2), lax.div(t, 2)], VT[t]
        scores = [_dot(k, q_s[at : at + STRIP, :], 1, 1) for at, _ in strips]
        weights, keeps = [], []
        for (at, masked), s in zip(strips, scores):
            if masked:
                gap = lax.broadcasted_iota(jnp.int32, (OWN, STRIP), 1) + at % OWN - lax.broadcasted_iota(jnp.int32, (OWN, STRIP), 0)
                s = jnp.where(gap >= 0, s, HIDDEN)
            old = top_s[:, at : at + STRIP]
            top = jnp.maximum(old, s.max(axis=0, keepdims=True))
            top_s[:, at : at + STRIP] = top
            weights.append(jnp.exp2((s - top) * e2).astype(jnp.bfloat16))
            keeps.append(jnp.exp2((old - top) * e2))
        for (at, _), p, keep in zip(strips, weights, keeps):
            mix_s[:, at : at + STRIP] = mix_s[:, at : at + STRIP] * keep + _dot(vt, p)

    first, second = range(0, OWN, STRIP), range(OWN, TOK, STRIP)

    def attend(h):
        top_s[...] = jnp.full((1, TOK), NEG, jnp.float32)
        mix_s[...] = jnp.zeros((HEAD + 8, TOK), jnp.float32)

        @pl.loop(0, low)
        def _(t):
            block(t, [(at, False) for at in (*first, *second)])

        block(low, [(at, True) for at in first] + [(at, False) for at in second])
        block(low + 1, [(at, False) for at in second])
        block(low + 2, [(at, True) for at in second])
        cols = pl.ds(pl.multiple_of(h * HEAD, HEAD), HEAD)
        for at in (*first, *second):
            total = mix_s[HEAD : HEAD + 1, at : at + STRIP]
            seen[at : at + STRIP, cols] = (mix_s[:HEAD, at : at + STRIP] * (1 / total)).T.astype(jnp.bfloat16)

    got_y(1)
    pass_x(1).start()
    pass_d(1, 1).start()
    stage_early(1)

    @pl.loop(1, G)
    def _(g):
        @pl.when(g + 3 < G)
        def _():
            own_y(g + 3).start()

        @pl.when(g + 1 < G)
        def _():
            got_y(g + 1)
            pass_x(g + 1).start()
            pass_d(g + 1, 1).start()

        @pl.when(g == G - 2)
        def _():
            @pl.loop(0, NC)
            def _(n):
                wo_x(n).start()
                wo_d(n).start()

        got_f(g)
        pass_d(g, 3).start()
        stage(g, 6).start()
        slot = lax.rem(g, 2)

        @pl.loop(0, 8)
        def _(b):
            @pl.when(b == 3)
            def _():
                got_d(g, 3)
                stage(g, 7).start()

            stage(g, b).wait()
            r = rows(mate(b))
            part = _dot(A[:, r], wbuf[slot, r, :])

            @pl.when(b == 0)
            def _():
                acc[...] = part

            @pl.when(b > 0)
            def _():
                acc[...] += part

        q_s[...] = _turn(acc[...].astype(jnp.bfloat16).astype(jnp.float32), cos[...], sin[...])

        @pl.when(g + 1 < G)
        def _():
            stage_early(g + 1)

        attend(g - 1)

    own_rows = pl.ds(pl.multiple_of(j * OWN, OWN), OWN)
    mate_rows = pl.ds(pl.multiple_of((1 - j) * OWN, OWN), OWN)
    own_slot, sib_slot = 2 * i + c, 2 * i + 1 - c
    x_slot, xs_slot = 2 * (1 - i) + c, 2 * (1 - i) + 1 - c

    def ocols(n):
        return pl.ds(pl.multiple_of(n * CW, CW), CW)

    def part_copy(n):
        return remote(pbuf.at[lax.rem(n, 2)], PR.at[n], sp.at[n], rp.at[n], yn)

    def part_in(n):
        return pltpu.make_async_copy(PR.at[n], prb.at[lax.rem(n, 2)], prs.at[lax.rem(n, 2)])

    def x_in(n):
        return pltpu.make_async_copy(x.at[:, ocols(n)], xb.at[lax.rem(n, 2)], xcs.at[lax.rem(n, 2)])

    def y_out(n):
        return pltpu.make_async_copy(yb.at[lax.rem(n, 2)], y.at[:, ocols(n)], ys.at[lax.rem(n, 2)])

    def ostage(n, s, k):
        return pltpu.make_async_copy(WO.at[n, rows(s), :], wob.at[lax.rem(n, 2), rows(s), :], wos.at[lax.rem(n, 2), k])

    def ostage_own(n):
        return pltpu.make_async_copy(wo.at[:, ocols(n)], wob.at[lax.rem(n, 2), rows(own_slot), :], wos.at[lax.rem(n, 2), 0])

    def take(n):
        part_copy(n).wait_recv()
        part_in(n).start()
        x_in(n).start()

    def finish(n):
        slot = lax.rem(n, 2)
        part_in(n).wait()
        x_in(n).wait()

        @pl.when(n >= 2)
        def _():
            y_out(n - 2).wait()

        yb[slot] = (xb[slot].astype(jnp.float32) + (obuf[lax.rem(n, 4)] + prb[slot])).astype(jnp.bfloat16)
        y_out(n).start()

    LAG = 3

    @pl.loop(0, NC)
    def _(n):
        slot = lax.rem(n, 2)
        ostage_own(n).start()
        remote(WO.at[n, rows(x_slot), :], WO.at[n, rows(x_slot), :], swx.at[n], rwx.at[n], xn).wait_recv()
        wo_pass(n).start()
        ostage(n, x_slot, 2).start()
        remote(WO.at[n, rows(sib_slot), :], WO.at[n, rows(sib_slot), :], swd.at[n, 0], rwd.at[n, 0], sib).wait_recv()
        ostage(n, sib_slot, 1).start()

        @pl.when(n >= LAG)
        def _():
            take(n - LAG)

        remote(WO.at[n, rows(xs_slot), :], WO.at[n, rows(xs_slot), :], swd.at[n, 1], rwd.at[n, 1], sib).wait_recv()
        ostage(n, xs_slot, 3).start()
        ostage_own(n).wait()
        for s, k in ((sib_slot, 1), (x_slot, 2), (xs_slot, 3)):
            ostage(n, s, k).wait()

        @pl.when(n >= 2)
        def _():
            part_copy(n - 2).wait_send()

        pbuf[slot] = _dot(seen[mate_rows, :], wob[slot])
        part_copy(n).start()
        obuf[lax.rem(n, 4)] = _dot(seen[own_rows, :], wob[slot])

        @pl.when(n >= LAG)
        def _():
            finish(n - LAG)

    for n in range(NC - LAG, NC):
        take(n)
        finish(n)
    for n in (NC - 2, NC - 1):
        y_out(n).wait()
        part_copy(n).wait_send()

    @pl.loop(0, G)
    def _(g):
        e = WQ.at[g, rows(me), :]
        remote(e, e, sy.at[g], ry.at[g], yn).wait_send()
        remote(e, e, sx.at[g], rx.at[g], xn).wait_send()
        remote(e, e, sf.at[g], rf.at[g], xn).wait_send()
        for kind in range(4):
            remote(e, e, sd.at[g, kind], rd.at[g, kind], sib).wait_send()

    for p in range(pieces):
        x_piece(p, j, yn).wait_send()
    for k, dev in enumerate((yn, xn, sib, yn, sib, sib, sib)):
        for which in range(2):
            kv_block(0, 0, 0, sk.at[k, which], dev).wait_send()

    @pl.loop(0, NC)
    def _(n):
        wo_x(n).wait_send()
        wo_d(n).wait_send()
        wo_pass(n).wait_send()


def solution(mesh):
    def step(x, gain, wq, wk, wv, wo):
        me = lax.axis_index("sp")
        low = me - 2 * ((me // 2) % 2)
        token = jnp.arange(OWN)
        place = jnp.concatenate([low * OWN + token, (low + 2) * OWN + token])
        half = HEAD // 2
        angle = place.astype(jnp.float32)[:, None] * THETA ** (-jnp.arange(half, dtype=jnp.float32) / half)
        bf16, f32, dma = jnp.bfloat16, jnp.float32, pltpu.SemaphoreType.DMA
        hbm, vmem = pl.BlockSpec(memory_space=pltpu.HBM), pl.BlockSpec(memory_space=pltpu.VMEM)
        out = pl.pallas_call(
            _kernel,
            out_shape=[
                jax.ShapeDtypeStruct((OWN, D), bf16),
                jax.ShapeDtypeStruct((G, D, HEAD), bf16),
                jax.ShapeDtypeStruct((NC, HEADS * HEAD, CW), bf16),
                jax.ShapeDtypeStruct((NC, OWN, CW), f32),
            ],
            in_specs=[hbm, vmem, hbm, hbm, hbm, vmem, vmem],
            out_specs=[hbm] * 4,
            scratch_shapes=[
                pltpu.VMEM((TOK, D), bf16),
                pltpu.VMEM((2, 2, 4, OWN, HEAD), bf16),
                pltpu.VMEM((8, HEAD + 8, OWN), bf16),
                pltpu.VMEM((TOK, HEADS * HEAD), bf16),
                pltpu.VMEM((2, D, HEAD), bf16),
                pltpu.VMEM((TOK, HEAD), bf16),
                pltpu.VMEM((TOK, HEAD), f32),
                pltpu.VMEM((1, TOK), f32),
                pltpu.VMEM((HEAD + 8, TOK), f32),
                pltpu.VMEM((2, HEADS * HEAD, CW), bf16),
                pltpu.VMEM((2, OWN, CW), f32),
                pltpu.VMEM((4, OWN, CW), f32),
                pltpu.VMEM((2, OWN, CW), f32),
                pltpu.VMEM((2, OWN, CW), bf16),
                pltpu.VMEM((2, OWN, CW), bf16),
                *[dma((G,))] * 6,
                *[dma((G, 4))] * 2,
                *[dma((OWN // PIECE,))] * 3,
                dma((7, 2)),
                dma((2, 2, 4)),
                dma((2, 8)),
                *[dma((NC,))] * 2,
                *[dma((NC, 2))] * 2,
                dma((2, 4)),
                *[dma((NC,))] * 2,
                *[dma((2,))] * 3,
            ],
            compiler_params=pltpu.CompilerParams(collective_id=0, has_side_effects=True, vmem_limit_bytes=VMEM),
            cost_estimate=pl.CostEstimate(flops=2 * 10**11, bytes_accessed=4 * 10**8, transcendentals=5 * 10**7),
        )(x, gain.reshape(1, D), jnp.concatenate([wk, wv], axis=1), wq, wo, jnp.cos(angle), jnp.sin(angle))
        return out[0]

    tokens, whole = P(("dp", "sp"), None), P("sp", None)
    return jax.shard_map(
        step,
        mesh=mesh,
        in_specs=(tokens, P(None), whole, whole, whole, whole),
        out_specs=tokens,
        check_vma=False,
    )
```

```python
import jax
import jax.numpy as jnp
import numpy as np
from jax import lax
from jax.experimental import pallas as pl
from jax.experimental.pallas import tpu as pltpu
from jax.sharding import PartitionSpec as P

HEAD = 256
HALF = HEAD // 2
THETA = 10000
NEG = -1e30
HIDDEN = 2 * NEG
LOG2E = 1.4426950408889634
MESH = pl.DeviceIdType.MESH
D = 8192
OWN = 512
TOK = 2 * OWN
ROWS = 1024
EARLY = 6 * ROWS
HEADS = 16
G = HEADS + 1
CW = 256
NC = D // CW
PIECE = 128
PIECES = OWN // PIECE
STRIP = 256
VMEM = 63 * 2**20


def _dot(a, b, ca=1, cb=0):
    return lax.dot_general(a, b, (((ca,), (cb,)), ((), ())), preferred_element_type=jnp.float32)


def _turn(t, cos, sin):
    a, b = t[:, :HALF], t[:, HALF:]
    return jnp.concatenate([a * cos - b * sin, b * cos + a * sin], axis=-1).astype(jnp.bfloat16)


def _kernel(x, gain, wk, wv, wq, wo, turns, y, WQ, WO, PR,
            A, KV, VT, seen, wbuf, q_s, acc, top_s, mix_s, wob, pbuf, obuf, prb, xb, yb, tab, cos, sin, gp,
            sn, rn, sm, rm, sf, rf, sd, rd, sxp, rxp, lxp, sk, rk, wst, swm, rwm, swd, rwd, wos, sp, rp, prs, xcs, ys, tabs):
    me = lax.axis_index("sp")
    j, i, c = lax.div(me, 4), lax.rem(lax.div(me, 2), 2), lax.rem(me, 2)
    sib, nb, mb = me + 1 - 2 * c, me + 4 - 8 * j, me + 2 - 4 * i

    def remote(src, dst, s, r, dev):
        return pltpu.make_async_remote_copy(src_ref=src, dst_ref=dst, send_sem=s, recv_sem=r, device_id={"sp": dev}, device_id_type=MESH)

    def local(src, dst, s):
        return pltpu.make_async_copy(src, dst, s)

    def rows(e):
        return pl.ds(pl.multiple_of(e * ROWS, ROWS), ROWS)

    def tokens(t):
        return pl.ds(pl.multiple_of(t * OWN, OWN), OWN)

    def qcols(jj, g):
        return pl.ds(pl.multiple_of(jj * (HEADS * HEAD) + (g - 1) * HEAD, HEAD), HEAD)

    def mate(b):
        b2, b1, b0 = b // 4, b // 2 % 2, b % 2
        return 4 * (j + b2 - 2 * j * b2) + 2 * (i + b1 - 2 * i * b1) + (c + b0 - 2 * c * b0)

    def own_n(g):
        return remote(wq.at[:, qcols(1 - j, g)], WQ.at[g, rows(me), :], sn.at[g], rn.at[g], nb)

    def own_m(g):
        return remote(wq.at[:, qcols(j, g)], WQ.at[g, rows(me), :], sm.at[g], rm.at[g], mb)

    def own_d(g):
        return remote(wq.at[:, qcols(j, g)], WQ.at[g, rows(me), :], sd.at[g, 0], rd.at[g, 0], sib)

    def moved(g, b, s, r, dev):
        here = WQ.at[g, rows(mate(b)), :]
        return remote(here, here, s, r, dev)

    def pass_m(g):
        return moved(g, 4, sf.at[g], rf.at[g], mb)

    def pass_d(g, kind):
        return moved(g, {1: 4, 2: 2, 3: 6}[kind], sd.at[g, kind], rd.at[g, kind], sib)

    def got_n(g):
        moved(g, 4, sn.at[g], rn.at[g], nb).wait_recv()

    def got_m(g):
        moved(g, 2, sm.at[g], rm.at[g], mb).wait_recv()

    def got_f(g):
        moved(g, 6, sf.at[g], rf.at[g], mb).wait_recv()

    def got_d(g, kind):
        moved(g, {0: 1, 1: 5, 2: 3, 3: 7}[kind], sd.at[g, kind], rd.at[g, kind], sib).wait_recv()

    def stage(g, b):
        slot = lax.rem(g, 2)
        return local(WQ.at[g, rows(mate(b)), :], wbuf.at[slot, b * ROWS : (b + 1) * ROWS, :], wst.at[slot, b])

    def stage_early(g):
        slot = lax.rem(g, 2)
        local(wq.at[:, qcols(j, g)], wbuf.at[slot, :ROWS, :], wst.at[slot, 0]).start()
        got_d(g, 0)
        stage(g, 1).start()
        stage(g, 2).start()
        got_d(g, 2)
        stage(g, 3).start()
        stage(g, 4).start()
        got_d(g, 1)
        stage(g, 5).start()

    def wo_m(n):
        return remote(wo.at[:, pl.ds(pl.multiple_of(n * CW, CW), CW)], WO.at[n, rows(2 * i + c), :], swm.at[n], rwm.at[n], mb)

    def wo_d(n):
        return remote(wo.at[:, pl.ds(pl.multiple_of(n * CW, CW), CW)], WO.at[n, rows(2 * i + c), :], swd.at[n, 0], rwd.at[n, 0], sib)

    def wo_pass(n):
        r = rows(2 * (1 - i) + c)
        return remote(WO.at[n, r, :], WO.at[n, r, :], swd.at[n, 1], rwd.at[n, 1], sib)

    def kv_block(kv, t, s, dev):
        return remote(KV.at[kv, tokens(t), :], KV.at[kv, tokens(t), :], s, rk.at[kv, t], dev)

    def x_place(p, jj):
        return pl.ds(pl.multiple_of(jj * OWN + p * PIECE, PIECE), PIECE)

    def x_send(p):
        for b in range(8):
            remote(x.at[pl.ds(p * PIECE, PIECE), rows(mate(b ^ 4))], A.at[x_place(p, j), b * ROWS : (b + 1) * ROWS], sxp.at[p], rxp.at[p], nb).start()

    def x_whole(p, jj):
        return remote(A.at[x_place(p, jj), :], A.at[x_place(p, jj), :], sxp.at[p], rxp.at[p], nb)

    barrier = pltpu.get_barrier_semaphore()
    for dev in (sib, nb, mb):
        pl.semaphore_signal(barrier, inc=1, device_id={"sp": dev}, device_id_type=MESH)
    pl.semaphore_wait(barrier, 3)

    def first_blocks(mine, other):
        remote(other, WQ.at[0, rows(me), :], sn.at[0], rn.at[0], nb).start()
        remote(mine, WQ.at[0, rows(me), :], sm.at[0], rm.at[0], mb).start()
        remote(mine, WQ.at[0, rows(me), :], sd.at[0, 0], rd.at[0, 0], sib).start()
        local(mine, wbuf.at[0, :ROWS, :], wst.at[0, 0]).start()

    @pl.when(j == 0)
    def _():
        first_blocks(wk, wv)

    @pl.when(j == 1)
    def _():
        first_blocks(wv, wk)

    x_send(0)
    x_send(1)
    own_m(1).start()
    for p in range(PIECES):
        for b in range(8):
            local(x.at[pl.ds(p * PIECE, PIECE), rows(mate(b))], A.at[x_place(p, j), b * ROWS : (b + 1) * ROWS], lxp.at[p]).start()
    local(turns, tab, tabs).start()

    @pl.loop(1, G)
    def _(g):
        own_d(g).start()

    for b in range(8):
        gp[:, b * ROWS : (b + 1) * ROWS] = gain[:, rows(mate(b))].astype(jnp.float32)

    local(turns, tab, tabs).wait()
    for jj in range(2):
        here = lax.broadcasted_iota(jnp.int32, (8, HEAD), 0) == 4 * jj + 2 * i + c
        turn = jnp.sum(jnp.where(here, tab[OWN:, :], 0.0), axis=0, keepdims=True)
        cr, sr, ct, st = tab[:OWN, :HALF], tab[:OWN, HALF:], turn[:, :HALF], turn[:, HALF:]
        cos[jj * OWN : (jj + 1) * OWN, :] = cr * ct - sr * st
        sin[jj * OWN : (jj + 1) * OWN, :] = sr * ct + cr * st

    got_n(0)
    pass_m(0).start()
    pass_d(0, 1).start()
    stage(0, 4).start()

    @pl.loop(2, 6)
    def _(g):
        own_m(g).start()

    got_m(0)
    pass_d(0, 2).start()
    stage(0, 2).start()
    got_f(0)
    pass_d(0, 3).start()
    stage(0, 6).start()
    for kind, b in ((0, 1), (2, 3), (1, 5), (3, 7)):
        got_d(0, kind)
        stage(0, b).start()
    for b in range(8):
        stage(0, b).wait()

    def norm_and_kv(p, jj):
        at = pl.multiple_of(jj * OWN + p * PIECE, PIECE)

        @pl.loop(0, PIECE // 16)
        def _(r):
            here = pl.ds(pl.multiple_of(at + r * 16, 16), 16)
            wide = A[here, :].astype(jnp.float32)
            scale = lax.rsqrt(jnp.mean(wide * wide, -1, keepdims=True) + 1e-6)
            A[here, :] = (wide * scale * gp[...]).astype(jnp.bfloat16)

        here = pl.ds(at, PIECE)
        t = _dot(A[here, :], wbuf[0]).astype(jnp.bfloat16)
        turned = _turn(t.astype(jnp.float32), cos[here, :], sin[here, :])
        first = pl.multiple_of((4 * jj + 2 * i + c) * OWN + p * PIECE, PIECE)
        KV[j, pl.ds(first, PIECE), :] = jnp.where(j == 0, turned, t)

    def kv_send(t, which):
        for k, dev in enumerate((nb, mb, sib)):
            kv_block(j, t, sk.at[k, which], dev).start()

    def kv_pass(t, which):
        kv_block(j, t, sk.at[3, which], mb).wait_recv()
        kv_block(j, t, sk.at[3, which], nb).start()
        kv_block(j, t, sk.at[4, which], sib).start()

    def relay(g):
        got_m(g)
        pass_d(g, 2).start()

    for p in range(PIECES):
        local(A.at[x_place(p, j), :], A.at[x_place(p, j), :], lxp.at[p]).wait()

    @pl.loop(0, PIECES)
    def _(p):
        norm_and_kv(p, j)

    kv_send(me, 0)
    x_send(2)

    @pl.loop(6, G)
    def _(g):
        own_m(g).start()

    @pl.loop(0, PIECES)
    def _(p):
        @pl.when(p == 2)
        def _():
            kv_pass(mb, 0)
            x_send(3)

        @pl.loop(3 * p + 1, 3 * p + 4)
        def _(g):
            relay(g)

        x_whole(p, 1 - j).wait_recv()
        norm_and_kv(p, 1 - j)

    kv_send(nb, 1)
    own_n(1).start()
    kv_pass(mate(6), 1)
    own_n(2).start()
    own_n(3).start()

    @pl.loop(3 * PIECES + 1, G)
    def _(g):
        relay(g)

    got_n(1)
    pass_m(1).start()
    pass_d(1, 1).start()
    stage_early(1)

    for which, b in enumerate((4, 6, 0, 2)):
        kv_block(1 - j, mate(b), sk.at[5, which % 2], nb).wait_recv()
        kv_block(1 - j, mate(b), sk.at[5 + which // 2, which % 2], sib).start()
    for kv in range(2):
        for b in (1, 3, 5, 7):
            kv_block(kv, mate(b), sk.at[6, 0], sib).wait_recv()

    @pl.loop(0, 8)
    def _(t):
        VT[:HEAD, tokens(t)] = KV[1, tokens(t), :].T
        VT[HEAD:, tokens(t)] = jnp.ones((8, OWN), jnp.bfloat16)

    e2 = HEAD**-0.5 * LOG2E
    low = 2 * i + c

    def step(work):
        scores = [_dot(KV[0, pl.ds(key, n), :], q_s[at : at + STRIP, :], 1, 1) for at, key, n, _ in work]
        weights, keeps = [], []
        for (at, key, n, cut), s in zip(work, scores):
            if cut:
                gap = lax.broadcasted_iota(jnp.int32, (OWN, STRIP), 1) + at % OWN - lax.broadcasted_iota(jnp.int32, (OWN, STRIP), 0)
                last = jnp.where(gap >= 0, s[n - OWN :], HIDDEN)
                s = last if n == OWN else jnp.concatenate([s[: n - OWN], last], axis=0)
            old = top_s[:, at : at + STRIP]
            top = jnp.maximum(old, s.max(axis=0, keepdims=True))
            top_s[:, at : at + STRIP] = top
            weights.append(jnp.exp2((s - top) * e2).astype(jnp.bfloat16))
            keeps.append(jnp.exp2((old - top) * e2))
        for (at, key, n, _), p, keep in zip(work, weights, keeps):
            mix_s[:, at : at + STRIP] = mix_s[:, at : at + STRIP] * keep + _dot(VT[:, pl.ds(key, n)], p)

    first, second = range(0, OWN, STRIP), range(OWN, TOK, STRIP)

    def attend(h):
        top_s[...] = jnp.full((1, TOK), NEG, jnp.float32)
        mix_s[...] = jnp.zeros((HEAD + 8, TOK), jnp.float32)

        @pl.loop(0, low)
        def _(t):
            key = pl.multiple_of(t * OWN, OWN)
            step([(at, key, OWN, False) for at in (*first, *second)])

        key = pl.multiple_of(low * OWN, OWN)
        step([(at, key, OWN, True) for at in first] + [(at, key, 2 * OWN, False) for at in second])
        key = pl.multiple_of((low + 2) * OWN, OWN)
        step([(at, key, 3 * OWN, True) for at in second])
        cols = pl.ds(pl.multiple_of(h * HEAD, HEAD), HEAD)
        for at in (*first, *second):
            total = mix_s[HEAD : HEAD + 1, at : at + STRIP]
            seen[at : at + STRIP, cols] = (mix_s[:HEAD, at : at + STRIP] * (1 / total)).T.astype(jnp.bfloat16)

    @pl.loop(1, G)
    def _(g):
        @pl.when(g + 3 < G)
        def _():
            own_n(g + 3).start()

        @pl.when(g + 1 < G)
        def _():
            got_n(g + 1)
            pass_m(g + 1).start()
            pass_d(g + 1, 1).start()

        @pl.when(g == G - 2)
        def _():
            @pl.loop(0, NC)
            def _(n):
                wo_m(n).start()
                wo_d(n).start()

        got_f(g)
        pass_d(g, 3).start()
        stage(g, 6).start()
        slot = lax.rem(g, 2)
        for b in range(6):
            stage(g, b).wait()
        acc[...] = _dot(A[:, :EARLY], wbuf[slot, :EARLY, :])
        got_d(g, 3)
        stage(g, 7).start()
        stage(g, 6).wait()
        stage(g, 7).wait()
        t = acc[...] + _dot(A[:, EARLY:], wbuf[slot, EARLY:, :])
        q_s[...] = _turn(t.astype(jnp.bfloat16).astype(jnp.float32), cos[...], sin[...])

        @pl.when(g + 1 < G)
        def _():
            stage_early(g + 1)

        attend(g - 1)

    own_rows = pl.ds(pl.multiple_of(j * OWN, OWN), OWN)
    mate_rows = pl.ds(pl.multiple_of((1 - j) * OWN, OWN), OWN)
    own_slot, sib_slot = 2 * i + c, 2 * i + 1 - c
    m_slot, ms_slot = 2 * (1 - i) + c, 2 * (1 - i) + 1 - c

    def ocols(n):
        return pl.ds(pl.multiple_of(n * CW, CW), CW)

    def part_copy(n):
        return remote(pbuf.at[lax.rem(n, 2)], PR.at[n], sp.at[n], rp.at[n], nb)

    def part_in(n):
        return pltpu.make_async_copy(PR.at[n], prb.at[lax.rem(n, 2)], prs.at[lax.rem(n, 2)])

    def x_in(n):
        return pltpu.make_async_copy(x.at[:, ocols(n)], xb.at[lax.rem(n, 2)], xcs.at[lax.rem(n, 2)])

    def y_out(n):
        return pltpu.make_async_copy(yb.at[lax.rem(n, 2)], y.at[:, ocols(n)], ys.at[lax.rem(n, 2)])

    def ostage(n, s, k):
        return pltpu.make_async_copy(WO.at[n, rows(s), :], wob.at[lax.rem(n, 2), rows(s), :], wos.at[lax.rem(n, 2), k])

    def ostage_own(n):
        return pltpu.make_async_copy(wo.at[:, ocols(n)], wob.at[lax.rem(n, 2), rows(own_slot), :], wos.at[lax.rem(n, 2), 0])

    def take(n):
        part_copy(n).wait_recv()
        part_in(n).start()
        x_in(n).start()

    def finish(n):
        slot = lax.rem(n, 2)
        part_in(n).wait()
        x_in(n).wait()

        @pl.when(n >= 2)
        def _():
            y_out(n - 2).wait()

        yb[slot] = (xb[slot].astype(jnp.float32) + (obuf[lax.rem(n, 4)] + prb[slot])).astype(jnp.bfloat16)
        y_out(n).start()

    LAG = 3

    @pl.loop(0, NC)
    def _(n):
        slot = lax.rem(n, 2)
        ostage_own(n).start()
        remote(WO.at[n, rows(m_slot), :], WO.at[n, rows(m_slot), :], swm.at[n], rwm.at[n], mb).wait_recv()
        wo_pass(n).start()
        ostage(n, m_slot, 2).start()
        remote(WO.at[n, rows(sib_slot), :], WO.at[n, rows(sib_slot), :], swd.at[n, 0], rwd.at[n, 0], sib).wait_recv()
        ostage(n, sib_slot, 1).start()

        @pl.when(n >= LAG)
        def _():
            take(n - LAG)

        remote(WO.at[n, rows(ms_slot), :], WO.at[n, rows(ms_slot), :], swd.at[n, 1], rwd.at[n, 1], sib).wait_recv()
        ostage(n, ms_slot, 3).start()
        ostage_own(n).wait()
        for s, k in ((sib_slot, 1), (m_slot, 2), (ms_slot, 3)):
            ostage(n, s, k).wait()

        @pl.when(n >= 2)
        def _():
            part_copy(n - 2).wait_send()

        pbuf[slot] = _dot(seen[mate_rows, :], wob[slot])
        part_copy(n).start()
        obuf[lax.rem(n, 4)] = _dot(seen[own_rows, :], wob[slot])

        @pl.when(n >= LAG)
        def _():
            finish(n - LAG)

    for n in range(NC - LAG, NC):
        take(n)
        finish(n)
    for n in (NC - 2, NC - 1):
        y_out(n).wait()
        part_copy(n).wait_send()

    @pl.loop(0, G)
    def _(g):
        for s, r, dev in ((sn.at[g], rn.at[g], nb), (sm.at[g], rm.at[g], mb), (sf.at[g], rf.at[g], mb)):
            moved(g, 0, s, r, dev).wait_send()
        for kind in range(4):
            moved(g, 0, sd.at[g, kind], rd.at[g, kind], sib).wait_send()

    for p in range(PIECES):
        x_whole(p, j).wait_send()
    for k, dev in enumerate((nb, mb, sib, nb, sib, sib, sib)):
        for which in range(2):
            kv_block(0, 0, sk.at[k, which], dev).wait_send()

    @pl.loop(0, NC)
    def _(n):
        wo_m(n).wait_send()
        wo_d(n).wait_send()
        wo_pass(n).wait_send()


def solution(mesh):
    def step(x, gain, wq, wk, wv, wo):
        rate = THETA ** (-np.arange(HALF) / HALF)
        angle = np.concatenate([np.arange(OWN), OWN * np.arange(8)])[:, None] * rate
        turns = np.concatenate([np.cos(angle), np.sin(angle)], axis=1).astype(np.float32)
        bf16, f32, dma = jnp.bfloat16, jnp.float32, pltpu.SemaphoreType.DMA
        hbm, vmem = pl.BlockSpec(memory_space=pltpu.HBM), pl.BlockSpec(memory_space=pltpu.VMEM)
        out = pl.pallas_call(
            _kernel,
            out_shape=[
                jax.ShapeDtypeStruct((OWN, D), bf16),
                jax.ShapeDtypeStruct((G, D, HEAD), bf16),
                jax.ShapeDtypeStruct((NC, HEADS * HEAD, CW), bf16),
                jax.ShapeDtypeStruct((NC, OWN, CW), f32),
            ],
            in_specs=[hbm, vmem, hbm, hbm, hbm, hbm, hbm],
            out_specs=[hbm] * 4,
            scratch_shapes=[
                pltpu.VMEM((TOK, D), bf16),
                pltpu.VMEM((2, 8 * OWN, HEAD), bf16),
                pltpu.VMEM((HEAD + 8, 8 * OWN), bf16),
                pltpu.VMEM((TOK, HEADS * HEAD), bf16),
                pltpu.VMEM((2, D, HEAD), bf16),
                pltpu.VMEM((TOK, HEAD), bf16),
                pltpu.VMEM((TOK, HEAD), f32),
                pltpu.VMEM((1, TOK), f32),
                pltpu.VMEM((HEAD + 8, TOK), f32),
                pltpu.VMEM((2, HEADS * HEAD, CW), bf16),
                pltpu.VMEM((2, OWN, CW), f32),
                pltpu.VMEM((4, OWN, CW), f32),
                pltpu.VMEM((2, OWN, CW), f32),
                pltpu.VMEM((2, OWN, CW), bf16),
                pltpu.VMEM((2, OWN, CW), bf16),
                pltpu.VMEM((OWN + 8, HEAD), f32),
                *[pltpu.VMEM((TOK, HALF), f32)] * 2,
                pltpu.VMEM((1, D), f32),
                *[dma((G,))] * 6,
                *[dma((G, 4))] * 2,
                *[dma((PIECES,))] * 3,
                dma((7, 2)),
                dma((2, 8)),
                dma((2, 8)),
                *[dma((NC,))] * 2,
                *[dma((NC, 2))] * 2,
                dma((2, 4)),
                *[dma((NC,))] * 2,
                *[dma((2,))] * 3,
                dma,
            ],
            compiler_params=pltpu.CompilerParams(collective_id=0, has_side_effects=True, vmem_limit_bytes=VMEM),
            cost_estimate=pl.CostEstimate(flops=2 * 10**11, bytes_accessed=4 * 10**8, transcendentals=5 * 10**7),
        )(x, gain.reshape(1, D), wk, wv, wq, wo, jnp.asarray(turns))
        return out[0]

    tokens, whole = P(("dp", "sp"), None), P("sp", None)
    return jax.shard_map(
        step,
        mesh=mesh,
        in_specs=(tokens, P(None), whole, whole, whole, whole),
        out_specs=tokens,
        check_vma=False,
    )
```

```python
import jax
import jax.numpy as jnp
import numpy as np
from jax import lax
from jax.experimental import pallas as pl
from jax.experimental.pallas import tpu as pltpu
from jax.sharding import PartitionSpec as P

HEAD = 256
HALF = HEAD // 2
THETA = 10000
NEG = -1e30
HIDDEN = 2 * NEG
LOG2E = 1.4426950408889634
MESH = pl.DeviceIdType.MESH
D = 8192
OWN = 512
TOK = 2 * OWN
ROWS = 1024
HEADS = 16
G = HEADS + 1
CW = 256
NC = D // CW - 1
PIECE = 128
PIECES = OWN // PIECE
STRIP = 256
VMEM = 63 * 2**20


def _dot(a, b, ca=1, cb=0):
    return lax.dot_general(a, b, (((ca,), (cb,)), ((), ())), preferred_element_type=jnp.float32)


def _turn(t, cos, sin):
    a, b = t[:, :HALF], t[:, HALF:]
    return jnp.concatenate([a * cos - b * sin, b * cos + a * sin], axis=-1).astype(jnp.bfloat16)


def _kernel(x, gain, wk, wv, wq, wo, turns, y, WQ, WO, PR,
            A, KV, VT, seen, wbuf, q_s, acc, top_s, mix_s, wob, obuf, prb, xb, yb, tab, cos, sin, gp,
            sn, rn, sm, rm, sf, rf, sd, rd, sxp, rxp, lxp, sk, rk, wst, swm, rwm, swd, rwd, wos, sp, rp, prs, xcs, ys, tabs):
    me = lax.axis_index("sp")
    j, i, c = lax.div(me, 4), lax.rem(lax.div(me, 2), 2), lax.rem(me, 2)
    sib, nb, mb = me + 1 - 2 * c, me + 4 - 8 * j, me + 2 - 4 * i

    def remote(src, dst, s, r, dev):
        return pltpu.make_async_remote_copy(src_ref=src, dst_ref=dst, send_sem=s, recv_sem=r, device_id={"sp": dev}, device_id_type=MESH)

    def local(src, dst, s):
        return pltpu.make_async_copy(src, dst, s)

    def rows(e):
        return pl.ds(pl.multiple_of(e * ROWS, ROWS), ROWS)

    def tokens(t):
        return pl.ds(pl.multiple_of(t * OWN, OWN), OWN)

    def qcols(jj, g):
        return pl.ds(pl.multiple_of(jj * (HEADS * HEAD) + (g - 1) * HEAD, HEAD), HEAD)

    def mate(b):
        b2, b1, b0 = b // 4, b // 2 % 2, b % 2
        return 4 * (j + b2 - 2 * j * b2) + 2 * (i + b1 - 2 * i * b1) + (c + b0 - 2 * c * b0)

    def half(e, k):
        return pl.ds(pl.multiple_of(e * ROWS + k * (ROWS // 2), ROWS // 2), ROWS // 2)

    def own_n(g):
        for k in range(2):
            src = wq.at[k * (ROWS // 2) : (k + 1) * (ROWS // 2), qcols(1 - j, g)]
            remote(src, WQ.at[g, half(me, k), :], sn.at[g, k], rn.at[g, k], nb).start()

    def own_m(g):
        return remote(wq.at[:, qcols(j, g)], WQ.at[g, rows(me), :], sm.at[g], rm.at[g], mb)

    def own_d(g):
        return remote(wq.at[:, qcols(j, g)], WQ.at[g, rows(me), :], sd.at[g, 0], rd.at[g, 0], sib)

    def moved(g, b, s, r, dev):
        here = WQ.at[g, rows(mate(b)), :]
        return remote(here, here, s, r, dev)

    def halved(g, b, k, s, r, dev):
        here = WQ.at[g, half(mate(b), k), :]
        return remote(here, here, s.at[g, k], r.at[g, k], dev)

    def relay_n(g, k):
        halved(g, 4, k, sn, rn, nb).wait_recv()
        halved(g, 4, k, sf, rf, mb).start()

    def pass_d(g, kind):
        return moved(g, {1: 4, 2: 2, 3: 6}[kind], sd.at[g, kind], rd.at[g, kind], sib)

    def got_m(g):
        moved(g, 2, sm.at[g], rm.at[g], mb).wait_recv()

    def got_f(g):
        for k in range(2):
            halved(g, 6, k, sf, rf, mb).wait_recv()

    def got_d(g, kind):
        moved(g, {0: 1, 1: 5, 2: 3, 3: 7}[kind], sd.at[g, kind], rd.at[g, kind], sib).wait_recv()

    def stage(g, b):
        slot = lax.rem(g, 2)
        return local(WQ.at[g, rows(mate(b)), :], wbuf.at[slot, b * ROWS : (b + 1) * ROWS, :], wst.at[slot, b])

    def stage_early(g):
        slot = lax.rem(g, 2)
        local(wq.at[:, qcols(j, g)], wbuf.at[slot, :ROWS, :], wst.at[slot, 0]).start()
        got_d(g, 0)
        stage(g, 1).start()
        stage(g, 2).start()
        got_d(g, 2)
        stage(g, 3).start()

    def block(n):
        return n, n, 0, CW

    tail = [(NC + k, NC, k * CW // 2, CW // 2) for k in range(2)]

    def wo_here(n, at, off, w):
        return wo.at[:, pl.ds(pl.multiple_of(at * CW + off, 128), w)]

    def wo_there(owner, n, at, off, w):
        return WO.at[at, rows(owner), off : off + w]

    def wo_m(k):
        return remote(wo_here(*k), wo_there(2 * i + c, *k), swm.at[k[0]], rwm.at[k[0]], mb)

    def wo_d(k):
        return remote(wo_here(*k), wo_there(2 * i + c, *k), swd.at[k[0], 0], rwd.at[k[0], 0], sib)

    def wo_pass(k):
        part = wo_there(2 * (1 - i) + c, *k)
        return remote(part, part, swd.at[k[0], 1], rwd.at[k[0], 1], sib)

    def kv_block(kv, t, s, dev):
        return remote(KV.at[kv, tokens(t), :], KV.at[kv, tokens(t), :], s, rk.at[kv, t], dev)

    def x_place(p, jj):
        return pl.ds(pl.multiple_of(jj * OWN + p * PIECE, PIECE), PIECE)

    def x_send(p):
        for b in range(8):
            remote(x.at[pl.ds(p * PIECE, PIECE), rows(mate(b ^ 4))], A.at[x_place(p, j), b * ROWS : (b + 1) * ROWS], sxp.at[p], rxp.at[p], nb).start()

    def x_whole(p, jj):
        return remote(A.at[x_place(p, jj), :], A.at[x_place(p, jj), :], sxp.at[p], rxp.at[p], nb)

    barrier = pltpu.get_barrier_semaphore()
    for dev in (sib, nb, mb):
        pl.semaphore_signal(barrier, inc=1, device_id={"sp": dev}, device_id_type=MESH)
    pl.semaphore_wait(barrier, 3)

    def first_blocks(mine, other):
        for k in range(2):
            remote(other.at[k * (ROWS // 2) : (k + 1) * (ROWS // 2), :], WQ.at[0, half(me, k), :], sn.at[0, k], rn.at[0, k], nb).start()
        remote(mine, WQ.at[0, rows(me), :], sm.at[0], rm.at[0], mb).start()
        remote(mine, WQ.at[0, rows(me), :], sd.at[0, 0], rd.at[0, 0], sib).start()
        local(mine, wbuf.at[0, :ROWS, :], wst.at[0, 0]).start()

    @pl.when(j == 0)
    def _():
        first_blocks(wk, wv)

    @pl.when(j == 1)
    def _():
        first_blocks(wv, wk)

    x_send(0)
    x_send(1)
    own_m(1).start()
    for p in range(PIECES):
        for b in range(8):
            local(x.at[pl.ds(p * PIECE, PIECE), rows(mate(b))], A.at[x_place(p, j), b * ROWS : (b + 1) * ROWS], lxp.at[p]).start()
    local(turns, tab, tabs).start()

    @pl.loop(1, G)
    def _(g):
        own_d(g).start()

    for b in range(8):
        gp[:, b * ROWS : (b + 1) * ROWS] = gain[rows(mate(b))].astype(jnp.float32).reshape(1, ROWS)

    local(turns, tab, tabs).wait()
    for jj in range(2):
        here = lax.broadcasted_iota(jnp.int32, (8, HEAD), 0) == 4 * jj + 2 * i + c
        turn = jnp.sum(jnp.where(here, tab[OWN:, :], 0.0), axis=0, keepdims=True)
        cr, sr, ct, st = tab[:OWN, :HALF], tab[:OWN, HALF:], turn[:, :HALF], turn[:, HALF:]
        cos[jj * OWN : (jj + 1) * OWN, :] = cr * ct - sr * st
        sin[jj * OWN : (jj + 1) * OWN, :] = sr * ct + cr * st

    relay_n(0, 0)
    relay_n(0, 1)
    pass_d(0, 1).start()
    stage(0, 4).start()

    @pl.loop(2, 6)
    def _(g):
        own_m(g).start()

    got_m(0)
    pass_d(0, 2).start()
    stage(0, 2).start()
    got_f(0)
    pass_d(0, 3).start()
    stage(0, 6).start()
    for kind, b in ((0, 1), (2, 3), (1, 5), (3, 7)):
        got_d(0, kind)
        stage(0, b).start()
    for b in range(8):
        stage(0, b).wait()

    def norm_and_kv(p, jj):
        at = pl.multiple_of(jj * OWN + p * PIECE, PIECE)

        @pl.loop(0, PIECE // 16)
        def _(r):
            here = pl.ds(pl.multiple_of(at + r * 16, 16), 16)
            wide = A[here, :].astype(jnp.float32)
            scale = lax.rsqrt(jnp.mean(wide * wide, -1, keepdims=True) + 1e-6)
            A[here, :] = (wide * scale * gp[...]).astype(jnp.bfloat16)

        here = pl.ds(at, PIECE)
        t = _dot(A[here, :], wbuf[0]).astype(jnp.bfloat16)
        turned = _turn(t.astype(jnp.float32), cos[here, :], sin[here, :])
        first = pl.multiple_of((4 * jj + 2 * i + c) * OWN + p * PIECE, PIECE)
        KV[j, pl.ds(first, PIECE), :] = jnp.where(j == 0, turned, t)

    def kv_send(t, which):
        for k, dev in enumerate((nb, mb, sib)):
            kv_block(j, t, sk.at[k, which], dev).start()

    def kv_pass(t, which):
        kv_block(j, t, sk.at[3, which], mb).wait_recv()
        kv_block(j, t, sk.at[3, which], nb).start()
        kv_block(j, t, sk.at[4, which], sib).start()

    def relay(g):
        got_m(g)
        pass_d(g, 2).start()

    for p in range(PIECES):
        local(A.at[x_place(p, j), :], A.at[x_place(p, j), :], lxp.at[p]).wait()

    @pl.loop(0, PIECES)
    def _(p):
        norm_and_kv(p, j)

    kv_send(me, 0)
    x_send(2)

    @pl.loop(0, NC)
    def _(n):
        wo_d(block(n)).start()

    for k in tail:
        wo_d(k).start()

    @pl.loop(6, G)
    def _(g):
        own_m(g).start()

    @pl.loop(0, PIECES)
    def _(p):
        @pl.when(p == 2)
        def _():
            kv_pass(mb, 0)
            x_send(3)
            own_n(1)

        @pl.loop(3 * p + 1, 3 * p + 4)
        def _(g):
            relay(g)

        x_whole(p, 1 - j).wait_recv()
        norm_and_kv(p, 1 - j)

    kv_send(nb, 1)
    wo_m(block(0)).start()
    kv_pass(mate(6), 1)
    own_n(2)
    own_n(3)

    @pl.loop(3 * PIECES + 1, G)
    def _(g):
        relay(g)

    relay_n(1, 0)
    relay_n(1, 1)
    pass_d(1, 1).start()
    stage_early(1)

    for which, b in enumerate((4, 6, 0, 2)):
        kv_block(1 - j, mate(b), sk.at[5, which % 2], nb).wait_recv()
        kv_block(1 - j, mate(b), sk.at[5 + which // 2, which % 2], sib).start()
    for kv in range(2):
        for b in (1, 3, 5, 7):
            kv_block(kv, mate(b), sk.at[6, 0], sib).wait_recv()

    relay_n(2, 0)

    @pl.loop(0, 8)
    def _(t):
        VT[:HEAD, tokens(t)] = KV[1, tokens(t), :].T
        VT[HEAD:, tokens(t)] = jnp.ones((8, OWN), jnp.bfloat16)

    e2 = HEAD**-0.5 * LOG2E
    low = 2 * i + c

    def step(work):
        scores = [_dot(KV[0, pl.ds(key, n), :], q_s[at : at + STRIP, :], 1, 1) for at, key, n, _ in work]
        weights, keeps = [], []
        for (at, key, n, cut), s in zip(work, scores):
            if cut:
                gap = lax.broadcasted_iota(jnp.int32, (OWN, STRIP), 1) + at % OWN - lax.broadcasted_iota(jnp.int32, (OWN, STRIP), 0)
                last = jnp.where(gap >= 0, s[n - OWN :], HIDDEN)
                s = last if n == OWN else jnp.concatenate([s[: n - OWN], last], axis=0)
            old = top_s[:, at : at + STRIP]
            top = jnp.maximum(old, s.max(axis=0, keepdims=True))
            top_s[:, at : at + STRIP] = top
            weights.append(jnp.exp2((s - top) * e2).astype(jnp.bfloat16))
            keeps.append(jnp.exp2((old - top) * e2))
        for (at, key, n, _), p, keep in zip(work, weights, keeps):
            mix_s[:, at : at + STRIP] = mix_s[:, at : at + STRIP] * keep + _dot(VT[:, pl.ds(key, n)], p)

    first, second = range(0, OWN, STRIP), range(OWN, TOK, STRIP)

    def attend(g):
        top_s[...] = jnp.full((1, TOK), NEG, jnp.float32)
        mix_s[...] = jnp.zeros((HEAD + 8, TOK), jnp.float32)

        @pl.loop(0, low)
        def _(t):
            key = pl.multiple_of(t * OWN, OWN)
            step([(at, key, OWN, False) for at in (*first, *second)])

        @pl.when(g + 2 < G)
        def _():
            relay_n(g + 2, 0)

        key = pl.multiple_of(low * OWN, OWN)
        step([(at, key, OWN, True) for at in first] + [(at, key, 2 * OWN, False) for at in second])
        key = pl.multiple_of((low + 2) * OWN, OWN)
        step([(at, key, 3 * OWN, True) for at in second])
        cols = pl.ds(pl.multiple_of((g - 1) * HEAD, HEAD), HEAD)
        for at in (*first, *second):
            total = mix_s[HEAD : HEAD + 1, at : at + STRIP]
            seen[at : at + STRIP, cols] = (mix_s[:HEAD, at : at + STRIP] * (1 / total)).T.astype(jnp.bfloat16)

    halves = [slice(0, OWN), slice(OWN, TOK)]

    own_rows = pl.ds(pl.multiple_of(j * OWN, OWN), OWN)
    mate_rows = pl.ds(pl.multiple_of((1 - j) * OWN, OWN), OWN)
    owners = [2 * i + c, 2 * i + 1 - c, 2 * (1 - i) + c, 2 * (1 - i) + 1 - c]

    def ring(n, size):
        return n % size if isinstance(n, int) else lax.rem(n, size)

    def ocols(n, at, off, w):
        return pl.ds(pl.multiple_of(at * CW + off, 128), w)

    def part_copy(k):
        n, at, off, w = k
        return remote(obuf.at[ring(n, 4), mate_rows, :w], PR.at[at, :, off : off + w], sp.at[n], rp.at[n], nb)

    def part_in(k):
        n, at, off, w = k
        return local(PR.at[at, :, off : off + w], prb.at[ring(n, 2), :, :w], prs.at[ring(n, 2)])

    def x_in(k):
        return local(x.at[:, ocols(*k)], xb.at[ring(k[0], 2), :, : k[3]], xcs.at[ring(k[0], 2)])

    def y_out(k):
        return local(yb.at[ring(k[0], 2), :, : k[3]], y.at[:, ocols(*k)], ys.at[ring(k[0], 2)])

    def ostage(k, o):
        src = wo_here(*k) if o == 0 else wo_there(owners[o], *k)
        return local(src, wob.at[ring(k[0], 2), rows(owners[o]), : k[3]], wos.at[ring(k[0], 2), o])

    def wo_got(k, o):
        part = wo_there(owners[o], *k)
        s, r, dev = {1: (swd.at[k[0], 0], rwd.at[k[0], 0], sib), 2: (swm.at[k[0]], rwm.at[k[0]], mb), 3: (swd.at[k[0], 1], rwd.at[k[0], 1], sib)}[o]
        remote(part, part, s, r, dev).wait_recv()

    def finish(k, before=None):
        n, _, _, w = k
        part_copy(k).wait_recv()
        part_in(k).start()
        x_in(k).start()
        if before is not None:
            y_out(before).wait()
        part_in(k).wait()
        x_in(k).wait()
        slot = ring(n, 2)
        yb[slot, :, :w] = (xb[slot, :, :w].astype(jnp.float32) + (obuf[ring(n, 4), own_rows, :w] + prb[slot, :, :w])).astype(jnp.bfloat16)
        y_out(k).start()

    def fetch(k):
        ostage(k, 0).start()
        wo_got(k, 2)
        wo_pass(k).start()
        ostage(k, 2).start()
        wo_got(k, 1)
        ostage(k, 1).start()
        wo_got(k, 3)
        ostage(k, 3).start()

    def multiply(k):
        n, _, _, w = k
        slot = ring(n, 2)
        for o in range(4):
            ostage(k, o).wait()
        if w == CW:
            obuf[ring(n, 4)] = _dot(seen[...], wob[slot])
        else:
            for r in halves:
                obuf[ring(n, 4), r, :w] = _dot(seen[r, :], wob[slot, :, :w])
        part_copy(k).start()

    @pl.loop(1, G)
    def _(g):
        @pl.when(g + 3 < G)
        def _():
            own_n(g + 3)

        got_f(g)
        pass_d(g, 3).start()
        stage(g, 6).start()
        stage(g, 4).start()
        got_d(g, 1)
        stage(g, 5).start()
        slot = lax.rem(g, 2)

        for b in range(4):
            stage(g, b).wait()
        for r in halves:
            acc[r, :] = _dot(A[r, : 4 * ROWS], wbuf[slot, : 4 * ROWS, :])

        @pl.when(g + 1 < G)
        def _():
            relay_n(g + 1, 1)
            pass_d(g + 1, 1).start()

        @pl.when(g == G - 2)
        def _():
            @pl.loop(1, NC)
            def _(n):
                wo_m(block(n)).start()

            for k in tail:
                wo_m(k).start()

        got_d(g, 3)
        stage(g, 7).start()
        stage(g, 4).wait()
        stage(g, 5).wait()
        for r in halves:
            acc[r, :] += _dot(A[r, 4 * ROWS : 6 * ROWS], wbuf[slot, 4 * ROWS : 6 * ROWS, :])
        stage(g, 6).wait()
        stage(g, 7).wait()
        for r in halves:
            t = acc[r, :] + _dot(A[r, 6 * ROWS :], wbuf[slot, 6 * ROWS :, :])
            q_s[r, :] = _turn(t.astype(jnp.bfloat16).astype(jnp.float32), cos[r, :], sin[r, :])

        @pl.when(g + 1 < G)
        def _():
            stage_early(g + 1)

        @pl.when(g == G - 1)
        def _():
            fetch(block(0))

        attend(g)

    @pl.loop(0, NC)
    def _(n):
        @pl.when(n >= 4)
        def _():
            part_copy(block(n - 4)).wait_send()

        @pl.when(n > 0)
        def _():
            fetch(block(n))

        multiply(block(n))

        @pl.when(n >= 4)
        def _():
            finish(block(n - 2), block(n - 4))

        @pl.when((n == 2) | (n == 3))
        def _():
            finish(block(n - 2))

    late = [block(n) for n in range(NC - 4, NC)] + tail
    for m in (4, 5):
        part_copy(late[m - 4]).wait_send()
        fetch(late[m])
        multiply(late[m])
        finish(late[m - 2], late[m - 4])
    for m in (4, 5):
        finish(late[m], late[m - 2])
    for m in (4, 5):
        y_out(late[m]).wait()
    for m in (2, 3, 4, 5):
        part_copy(late[m]).wait_send()

    @pl.loop(0, G)
    def _(g):
        moved(g, 0, sm.at[g], rm.at[g], mb).wait_send()
        for k in range(2):
            halved(g, 0, k, sn, rn, nb).wait_send()
            halved(g, 0, k, sf, rf, mb).wait_send()
        for kind in range(4):
            moved(g, 0, sd.at[g, kind], rd.at[g, kind], sib).wait_send()

    for p in range(PIECES):
        x_whole(p, j).wait_send()
    for k, dev in enumerate((nb, mb, sib, nb, sib, sib, sib)):
        for which in range(2):
            kv_block(0, 0, sk.at[k, which], dev).wait_send()

    @pl.loop(0, NC)
    def _(n):
        for f in (wo_m, wo_d, wo_pass):
            f(block(n)).wait_send()

    for k in tail:
        for f in (wo_m, wo_d, wo_pass):
            f(k).wait_send()


def solution(mesh):
    def step(x, gain, wq, wk, wv, wo):
        rate = THETA ** (-np.arange(HALF) / HALF)
        angle = np.concatenate([np.arange(OWN), OWN * np.arange(8)])[:, None] * rate
        turns = np.concatenate([np.cos(angle), np.sin(angle)], axis=1).astype(np.float32)
        bf16, f32, dma = jnp.bfloat16, jnp.float32, pltpu.SemaphoreType.DMA
        hbm, vmem = pl.BlockSpec(memory_space=pltpu.HBM), pl.BlockSpec(memory_space=pltpu.VMEM)
        out = pl.pallas_call(
            _kernel,
            out_shape=[
                jax.ShapeDtypeStruct((OWN, D), bf16),
                jax.ShapeDtypeStruct((G, D, HEAD), bf16),
                jax.ShapeDtypeStruct((NC + 1, HEADS * HEAD, CW), bf16),
                jax.ShapeDtypeStruct((NC + 1, OWN, CW), f32),
            ],
            in_specs=[hbm, vmem, hbm, hbm, hbm, hbm, hbm],
            out_specs=[hbm] * 4,
            scratch_shapes=[
                pltpu.VMEM((TOK, D), bf16),
                pltpu.VMEM((2, 8 * OWN, HEAD), bf16),
                pltpu.VMEM((HEAD + 8, 8 * OWN), bf16),
                pltpu.VMEM((TOK, HEADS * HEAD), bf16),
                pltpu.VMEM((2, D, HEAD), bf16),
                pltpu.VMEM((TOK, HEAD), bf16),
                pltpu.VMEM((TOK, HEAD), f32),
                pltpu.VMEM((1, TOK), f32),
                pltpu.VMEM((HEAD + 8, TOK), f32),
                pltpu.VMEM((2, HEADS * HEAD, CW), bf16),
                pltpu.VMEM((4, TOK, CW), f32),
                pltpu.VMEM((2, OWN, CW), f32),
                pltpu.VMEM((2, OWN, CW), bf16),
                pltpu.VMEM((2, OWN, CW), bf16),
                pltpu.VMEM((OWN + 8, HEAD), f32),
                *[pltpu.VMEM((TOK, HALF), f32)] * 2,
                pltpu.VMEM((1, D), f32),
                *[dma((G, 2))] * 2,
                *[dma((G,))] * 2,
                *[dma((G, 2))] * 2,
                *[dma((G, 4))] * 2,
                *[dma((PIECES,))] * 3,
                dma((7, 2)),
                dma((2, 8)),
                dma((2, 8)),
                *[dma((NC + 2,))] * 2,
                *[dma((NC + 2, 2))] * 2,
                dma((2, 4)),
                *[dma((NC + 2,))] * 2,
                *[dma((2,))] * 3,
                dma,
            ],
            compiler_params=pltpu.CompilerParams(collective_id=0, has_side_effects=True, vmem_limit_bytes=VMEM),
            cost_estimate=pl.CostEstimate(flops=2 * 10**11, bytes_accessed=4 * 10**8, transcendentals=5 * 10**7),
        )(x, gain, wk, wv, wq, wo, jnp.asarray(turns))
        return out[0]

    tokens, whole = P(("dp", "sp"), None), P("sp", None)
    return jax.shard_map(
        step,
        mesh=mesh,
        in_specs=(tokens, P(None), whole, whole, whole, whole),
        out_specs=tokens,
        check_vma=False,
    )
```

```python
import jax
import jax.numpy as jnp
import numpy as np
from jax import lax
from jax.experimental import pallas as pl
from jax.experimental.pallas import tpu as pltpu
from jax.sharding import PartitionSpec as P

HEAD = 256
HALF = HEAD // 2
THETA = 10000
NEG = -1e30
HIDDEN = 2 * NEG
LOG2E = 1.4426950408889634
MESH = pl.DeviceIdType.MESH
D = 8192
OWN = 512
TOK = 2 * OWN
ROWS = 1024
HEADS = 16
G = HEADS + 1
CW = 256
NC = D // CW - 1
PIECE = 128
PIECES = OWN // PIECE
STRIP = 256
VMEM = 63 * 2**20


def _dot(a, b, ca=1, cb=0):
    return lax.dot_general(a, b, (((ca,), (cb,)), ((), ())), preferred_element_type=jnp.float32)


def _turn(t, cos, sin):
    a, b = t[:, :HALF], t[:, HALF:]
    return jnp.concatenate([a * cos - b * sin, b * cos + a * sin], axis=-1).astype(jnp.bfloat16)


def _kernel(x, gain, wk, wv, wq, wo, turns, y, WQ, WO, PR, SQ, SO,
            A, KV, VT, seen, wbuf, q_s, acc, top_s, mix_s, wob, obuf, prb, plast, xb, yb, tab, cos, sin, gp,
            sn, rn, sm, rm, sf, rf, sd, rd, so, ro, sxp, rxp, lxp, sk, rk, wst, swm, rwm, swd, rwd, wos, sp, rp, prs, xcs, ys, tabs):
    me = lax.axis_index("sp")
    j, i, c = lax.div(me, 4), lax.rem(lax.div(me, 2), 2), lax.rem(me, 2)
    sib, nb, mb = me + 1 - 2 * c, me + 4 - 8 * j, me + 2 - 4 * i

    def remote(src, dst, s, r, dev):
        return pltpu.make_async_remote_copy(src_ref=src, dst_ref=dst, send_sem=s, recv_sem=r, device_id={"sp": dev}, device_id_type=MESH)

    def local(src, dst, s):
        return pltpu.make_async_copy(src, dst, s)

    def rows(e):
        return pl.ds(pl.multiple_of(e * ROWS, ROWS), ROWS)

    def tokens(t):
        return pl.ds(pl.multiple_of(t * OWN, OWN), OWN)

    def qcols(jj, g):
        return pl.ds(pl.multiple_of(jj * (HEADS * HEAD) + (g - 1) * HEAD, HEAD), HEAD)

    def mate(b):
        b2, b1, b0 = b // 4, b // 2 % 2, b % 2
        return 4 * (j + b2 - 2 * j * b2) + 2 * (i + b1 - 2 * i * b1) + (c + b0 - 2 * c * b0)

    def half(e, k):
        return pl.ds(pl.multiple_of(e * ROWS + k * (ROWS // 2), ROWS // 2), ROWS // 2)

    def own_n(g):
        for k in range(2):
            src = wq.at[k * (ROWS // 2) : (k + 1) * (ROWS // 2), qcols(1 - j, g)]
            remote(src, WQ.at[g, half(me, k), :], sn, rn.at[g, k], nb).start()

    def own_m(g):
        return remote(wq.at[:, qcols(j, g)], WQ.at[g, rows(me), :], sm, rm.at[g], mb)

    def own_d():
        return remote(wq.at[:, pl.ds(pl.multiple_of(j * HEADS * HEAD, HEAD), HEADS * HEAD)], SQ, so.at[0], ro.at[0], sib)

    def wo_d():
        return remote(wo, SO, so.at[1], ro.at[1], sib)

    def moved(g, b, s, r, dev):
        here = WQ.at[g, rows(mate(b)), :]
        return remote(here, here, s, r, dev)

    def halved(g, b, k, s, r, dev):
        here = WQ.at[g, half(mate(b), k), :]
        return remote(here, here, s, r.at[g, k], dev)

    def relay_n(g, k):
        halved(g, 4, k, sn, rn, nb).wait_recv()
        halved(g, 4, k, sf, rf, mb).start()

    def pass_d(g, kind):
        return moved(g, {1: 4, 2: 2, 3: 6}[kind], sd.at[kind], rd.at[g, kind - 1], sib)

    def got_m(g):
        moved(g, 2, sm, rm.at[g], mb).wait_recv()

    def got_f(g):
        for k in range(2):
            halved(g, 6, k, sf, rf, mb).wait_recv()

    def got_d(g, kind):
        moved(g, {1: 5, 2: 3, 3: 7}[kind], sd.at[kind], rd.at[g, kind - 1], sib).wait_recv()

    def stage(g, b):
        slot = lax.rem(g, 2)
        return local(WQ.at[g, rows(mate(b)), :], wbuf.at[slot, b * ROWS : (b + 1) * ROWS, :], wst.at[slot, b])

    def stage_early(g):
        slot = lax.rem(g, 2)
        local(wq.at[:, qcols(j, g)], wbuf.at[slot, :ROWS, :], wst.at[slot, 0]).start()
        local(SQ.at[:, pl.ds(pl.multiple_of((g - 1) * HEAD, HEAD), HEAD)], wbuf.at[slot, ROWS : 2 * ROWS, :], wst.at[slot, 1]).start()
        stage(g, 2).start()
        got_d(g, 2)
        stage(g, 3).start()

    def block(n):
        return n, n, 0, CW

    tail = [(NC + k, NC, k * CW // 2, CW // 2) for k in range(2)]

    def wo_here(n, at, off, w):
        return wo.at[:, pl.ds(pl.multiple_of(at * CW + off, 128), w)]

    def wo_there(owner, n, at, off, w):
        return WO.at[at, rows(owner), off : off + w]

    def wo_m(k):
        return remote(wo_here(*k), wo_there(2 * i + c, *k), swm, rwm.at[k[0]], mb)

    def wo_pass(k):
        part = wo_there(2 * (1 - i) + c, *k)
        return remote(part, part, swd, rwd.at[k[0]], sib)

    def kv_block(kv, t, s, dev):
        return remote(KV.at[kv, tokens(t), :], KV.at[kv, tokens(t), :], s, rk.at[kv, t], dev)

    def x_place(p, jj):
        return pl.ds(pl.multiple_of(jj * OWN + p * PIECE, PIECE), PIECE)

    def x_send(p):
        for b in range(8):
            remote(x.at[pl.ds(p * PIECE, PIECE), rows(mate(b ^ 4))], A.at[x_place(p, j), b * ROWS : (b + 1) * ROWS], sxp.at[p], rxp.at[p], nb).start()

    def x_whole(p, jj):
        return remote(A.at[x_place(p, jj), :], A.at[x_place(p, jj), :], sxp.at[p], rxp.at[p], nb)

    barrier = pltpu.get_barrier_semaphore()
    for dev in (sib, nb, mb):
        pl.semaphore_signal(barrier, inc=1, device_id={"sp": dev}, device_id_type=MESH)
    pl.semaphore_wait(barrier, 3)

    def first_blocks(mine, other):
        for k in range(2):
            remote(other.at[k * (ROWS // 2) : (k + 1) * (ROWS // 2), :], WQ.at[0, half(me, k), :], sn, rn.at[0, k], nb).start()
        remote(mine, WQ.at[0, rows(me), :], sm, rm.at[0], mb).start()
        remote(mine, WQ.at[0, rows(me), :], sd.at[0], ro.at[2], sib).start()
        local(mine, wbuf.at[0, :ROWS, :], wst.at[0, 0]).start()

    @pl.when(j == 0)
    def _():
        first_blocks(wk, wv)

    @pl.when(j == 1)
    def _():
        first_blocks(wv, wk)

    x_send(0)
    x_send(1)
    own_m(1).start()
    for p in range(PIECES):
        for b in range(8):
            local(x.at[pl.ds(p * PIECE, PIECE), rows(mate(b))], A.at[x_place(p, j), b * ROWS : (b + 1) * ROWS], lxp.at[p]).start()
    local(turns, tab, tabs).start()

    own_d().start()

    for b in range(8):
        gp[:, b * ROWS : (b + 1) * ROWS] = gain[rows(mate(b))].astype(jnp.float32).reshape(1, ROWS)

    local(turns, tab, tabs).wait()
    for jj in range(2):
        here = lax.broadcasted_iota(jnp.int32, (8, HEAD), 0) == 4 * jj + 2 * i + c
        turn = jnp.sum(jnp.where(here, tab[OWN:, :], 0.0), axis=0, keepdims=True)
        cr, sr, ct, st = tab[:OWN, :HALF], tab[:OWN, HALF:], turn[:, :HALF], turn[:, HALF:]
        cos[jj * OWN : (jj + 1) * OWN, :] = cr * ct - sr * st
        sin[jj * OWN : (jj + 1) * OWN, :] = sr * ct + cr * st

    relay_n(0, 0)
    relay_n(0, 1)
    pass_d(0, 1).start()
    stage(0, 4).start()

    @pl.loop(2, 6)
    def _(g):
        own_m(g).start()

    got_m(0)
    pass_d(0, 2).start()
    stage(0, 2).start()
    got_f(0)
    pass_d(0, 3).start()
    stage(0, 6).start()
    moved(0, 1, sd.at[0], ro.at[2], sib).wait_recv()
    stage(0, 1).start()
    for kind, b in ((2, 3), (1, 5), (3, 7)):
        got_d(0, kind)
        stage(0, b).start()
    for b in range(8):
        stage(0, b).wait()

    def norm_and_kv(p, jj):
        at = pl.multiple_of(jj * OWN + p * PIECE, PIECE)

        @pl.loop(0, PIECE // 16)
        def _(r):
            here = pl.ds(pl.multiple_of(at + r * 16, 16), 16)
            wide = A[here, :].astype(jnp.float32)
            scale = lax.rsqrt(jnp.mean(wide * wide, -1, keepdims=True) + 1e-6)
            A[here, :] = (wide * scale * gp[...]).astype(jnp.bfloat16)

        here = pl.ds(at, PIECE)
        t = _dot(A[here, :], wbuf[0]).astype(jnp.bfloat16)
        turned = _turn(t.astype(jnp.float32), cos[here, :], sin[here, :])
        first = pl.multiple_of((4 * jj + 2 * i + c) * OWN + p * PIECE, PIECE)
        KV[j, pl.ds(first, PIECE), :] = jnp.where(j == 0, turned, t)

    def kv_send(t, which):
        for k, dev in enumerate((nb, mb, sib)):
            kv_block(j, t, sk.at[k, which], dev).start()

    def kv_pass(t, which):
        kv_block(j, t, sk.at[3, which], mb).wait_recv()
        kv_block(j, t, sk.at[3, which], nb).start()
        kv_block(j, t, sk.at[4, which], sib).start()

    def relay(g):
        got_m(g)
        pass_d(g, 2).start()

    for p in range(PIECES):
        local(A.at[x_place(p, j), :], A.at[x_place(p, j), :], lxp.at[p]).wait()

    @pl.loop(0, PIECES)
    def _(p):
        norm_and_kv(p, j)

    kv_send(me, 0)
    x_send(2)

    wo_d().start()

    @pl.loop(6, G)
    def _(g):
        own_m(g).start()

    @pl.loop(0, PIECES)
    def _(p):
        @pl.when(p == 2)
        def _():
            kv_pass(mb, 0)
            x_send(3)
            own_n(1)

        @pl.loop(3 * p + 1, 3 * p + 4)
        def _(g):
            relay(g)

        x_whole(p, 1 - j).wait_recv()
        norm_and_kv(p, 1 - j)

    kv_send(nb, 1)
    wo_m(block(0)).start()
    kv_pass(mate(6), 1)
    own_n(2)
    own_n(3)

    @pl.loop(3 * PIECES + 1, G)
    def _(g):
        relay(g)

    own_d().wait_recv()
    wo_d().wait_recv()
    relay_n(1, 0)
    relay_n(1, 1)
    pass_d(1, 1).start()
    stage_early(1)

    for which, b in enumerate((4, 6, 0, 2)):
        kv_block(1 - j, mate(b), sk.at[5, which % 2], nb).wait_recv()
        kv_block(1 - j, mate(b), sk.at[5 + which // 2, which % 2], sib).start()
    for kv in range(2):
        for b in (1, 3, 5, 7):
            kv_block(kv, mate(b), sk.at[6, 0], sib).wait_recv()

    relay_n(2, 0)

    @pl.loop(0, 8)
    def _(t):
        VT[:HEAD, tokens(t)] = KV[1, tokens(t), :].T
        VT[HEAD:, tokens(t)] = jnp.ones((8, OWN), jnp.bfloat16)

    e2 = HEAD**-0.5 * LOG2E
    low = 2 * i + c

    def step(work):
        scores = [_dot(KV[0, pl.ds(key, n), :], q_s[at : at + STRIP, :], 1, 1) for at, key, n, _ in work]
        weights, keeps = [], []
        for (at, key, n, cut), s in zip(work, scores):
            if cut:
                gap = lax.broadcasted_iota(jnp.int32, (OWN, STRIP), 1) + at % OWN - lax.broadcasted_iota(jnp.int32, (OWN, STRIP), 0)
                last = jnp.where(gap >= 0, s[n - OWN :], HIDDEN)
                s = last if n == OWN else jnp.concatenate([s[: n - OWN], last], axis=0)
            old = top_s[:, at : at + STRIP]
            top = jnp.maximum(old, s.max(axis=0, keepdims=True))
            top_s[:, at : at + STRIP] = top
            weights.append(jnp.exp2((s - top) * e2).astype(jnp.bfloat16))
            keeps.append(jnp.exp2((old - top) * e2))
        for (at, key, n, _), p, keep in zip(work, weights, keeps):
            mix_s[:, at : at + STRIP] = mix_s[:, at : at + STRIP] * keep + _dot(VT[:, pl.ds(key, n)], p)

    first, second = range(0, OWN, STRIP), range(OWN, TOK, STRIP)

    def attend(g):
        top_s[...] = jnp.full((1, TOK), NEG, jnp.float32)
        mix_s[...] = jnp.zeros((HEAD + 8, TOK), jnp.float32)

        @pl.loop(0, low)
        def _(t):
            key = pl.multiple_of(t * OWN, OWN)
            step([(at, key, OWN, False) for at in (*first, *second)])

        @pl.when(g + 2 < G)
        def _():
            relay_n(g + 2, 0)

        key = pl.multiple_of(low * OWN, OWN)
        step([(at, key, OWN, True) for at in first] + [(at, key, 2 * OWN, False) for at in second])
        key = pl.multiple_of((low + 2) * OWN, OWN)
        step([(at, key, 3 * OWN, True) for at in second])
        cols = pl.ds(pl.multiple_of((g - 1) * HEAD, HEAD), HEAD)
        for at in (*first, *second):
            total = mix_s[HEAD : HEAD + 1, at : at + STRIP]
            seen[at : at + STRIP, cols] = (mix_s[:HEAD, at : at + STRIP] * (1 / total)).T.astype(jnp.bfloat16)

    halves = [slice(0, OWN), slice(OWN, TOK)]

    own_rows = pl.ds(pl.multiple_of(j * OWN, OWN), OWN)
    mate_rows = pl.ds(pl.multiple_of((1 - j) * OWN, OWN), OWN)
    owners = [2 * i + c, 2 * i + 1 - c, 2 * (1 - i) + c, 2 * (1 - i) + 1 - c]

    def ring(n, size):
        return n % size if isinstance(n, int) else lax.rem(n, size)

    def ocols(n, at, off, w):
        return pl.ds(pl.multiple_of(at * CW + off, 128), w)

    def part_copy(k):
        n, at, off, w = k
        dst = PR.at[at] if w == CW else plast.at[n - NC]
        return remote(obuf.at[ring(n, 4), mate_rows, :w], dst, sp.at[ring(n, 4)], rp.at[n], nb)

    def part_in(k):
        n, at, _, _ = k
        return local(PR.at[at], prb.at[ring(n, 2)], prs.at[ring(n, 2)])

    def x_in(k):
        return local(x.at[:, ocols(*k)], xb.at[ring(k[0], 2), :, : k[3]], xcs.at[ring(k[0], 2)])

    def y_out(k):
        return local(yb.at[ring(k[0], 2), :, : k[3]], y.at[:, ocols(*k)], ys.at[ring(k[0], 2)])

    def ostage(k, o):
        src = wo_here(*k) if o == 0 else SO.at[:, ocols(*k)] if o == 1 else wo_there(owners[o], *k)
        return local(src, wob.at[ring(k[0], 2), rows(owners[o]), : k[3]], wos.at[ring(k[0], 2), o])

    def wo_got(k, o):
        part = wo_there(owners[o], *k)
        s, r, dev = (swm, rwm.at[k[0]], mb) if o == 2 else (swd, rwd.at[k[0]], sib)
        remote(part, part, s, r, dev).wait_recv()

    def finish(k, before=None):
        n, _, _, w = k
        slot = ring(n, 2)
        x_in(k).start()
        part_copy(k).wait_recv()
        if w == CW:
            part_in(k).start()
            part_in(k).wait()
        if before is not None:
            y_out(before).wait()
        x_in(k).wait()
        part = prb[slot] if w == CW else plast[n - NC]
        yb[slot, :, :w] = (xb[slot, :, :w].astype(jnp.float32) + (obuf[ring(n, 4), own_rows, :w] + part)).astype(jnp.bfloat16)
        y_out(k).start()

    def share(k):
        wo_got(k, 2)
        wo_pass(k).start()

    def fetch(k):
        ostage(k, 0).start()
        ostage(k, 1).start()
        if not isinstance(k[0], int) or k[0] > 0:
            share(k)
        ostage(k, 2).start()
        wo_got(k, 3)
        ostage(k, 3).start()

    def multiply(k):
        n, _, _, w = k
        slot = ring(n, 2)
        for o in range(4):
            ostage(k, o).wait()
        if w == CW:
            obuf[ring(n, 4)] = _dot(seen[...], wob[slot])
        else:
            for r in halves:
                obuf[ring(n, 4), r, :w] = _dot(seen[r, :], wob[slot, :, :w])
        part_copy(k).start()

    @pl.loop(1, G)
    def _(g):
        @pl.when(g + 3 < G)
        def _():
            own_n(g + 3)

        got_f(g)
        pass_d(g, 3).start()
        stage(g, 6).start()
        stage(g, 4).start()
        got_d(g, 1)
        stage(g, 5).start()
        slot = lax.rem(g, 2)

        for b in range(4):
            stage(g, b).wait()
        for r in halves:
            acc[r, :] = _dot(A[r, : 4 * ROWS], wbuf[slot, : 4 * ROWS, :])

        @pl.when(g + 1 < G)
        def _():
            relay_n(g + 1, 1)
            pass_d(g + 1, 1).start()

        @pl.when(g == G - 2)
        def _():
            @pl.loop(1, NC)
            def _(n):
                wo_m(block(n)).start()

            for k in tail:
                wo_m(k).start()

        got_d(g, 3)
        stage(g, 7).start()
        stage(g, 4).wait()
        stage(g, 5).wait()
        for r in halves:
            acc[r, :] += _dot(A[r, 4 * ROWS : 6 * ROWS], wbuf[slot, 4 * ROWS : 6 * ROWS, :])
        stage(g, 6).wait()
        stage(g, 7).wait()
        for r in halves:
            t = acc[r, :] + _dot(A[r, 6 * ROWS :], wbuf[slot, 6 * ROWS :, :])
            q_s[r, :] = _turn(t.astype(jnp.bfloat16).astype(jnp.float32), cos[r, :], sin[r, :])

        @pl.when(g + 1 < G)
        def _():
            stage_early(g + 1)

        @pl.when(g == HEADS // 2)
        def _():
            share(block(0))

        @pl.when(g == G - 1)
        def _():
            fetch(block(0))

        attend(g)

    @pl.loop(0, NC)
    def _(n):
        @pl.when(n >= 4)
        def _():
            part_copy(block(n - 4)).wait_send()

        @pl.when(n > 0)
        def _():
            fetch(block(n))

        multiply(block(n))

        @pl.when(n >= 4)
        def _():
            finish(block(n - 2), block(n - 4))

        @pl.when((n == 2) | (n == 3))
        def _():
            finish(block(n - 2))

    late = [block(n) for n in range(NC - 4, NC)] + tail
    for m in (4, 5):
        part_copy(late[m - 4]).wait_send()
        fetch(late[m])
        multiply(late[m])
        finish(late[m - 2], late[m - 4])
    for m in (4, 5):
        finish(late[m], late[m - 2])
    for m in (4, 5):
        y_out(late[m]).wait()
    for m in (2, 3, 4, 5):
        part_copy(late[m]).wait_send()

    sent = WQ.at[:, rows(0), :]
    for k, dev in ((sn, nb), (sm, mb), (sf, mb), (sd.at[1], sib), (sd.at[2], sib), (sd.at[3], sib)):
        remote(sent, sent, k, rm.at[0], dev).wait_send()
    moved(0, 0, sd.at[0], rm.at[0], sib).wait_send()
    own_d().wait_send()
    wo_d().wait_send()
    sent = WO.at[:, rows(0), :]
    for k, dev in ((swm, mb), (swd, sib)):
        remote(sent, sent, k, rm.at[0], dev).wait_send()
    for p in range(PIECES):
        x_whole(p, j).wait_send()
    for k, dev in enumerate((nb, mb, sib, nb, sib, sib, sib)):
        for which in range(2):
            kv_block(0, 0, sk.at[k, which], dev).wait_send()


def solution(mesh):
    def step(x, gain, wq, wk, wv, wo):
        rate = THETA ** (-np.arange(HALF) / HALF)
        angle = np.concatenate([np.arange(OWN), OWN * np.arange(8)])[:, None] * rate
        turns = np.concatenate([np.cos(angle), np.sin(angle)], axis=1).astype(np.float32)
        bf16, f32, dma = jnp.bfloat16, jnp.float32, pltpu.SemaphoreType.DMA
        hbm, vmem = pl.BlockSpec(memory_space=pltpu.HBM), pl.BlockSpec(memory_space=pltpu.VMEM)
        out = pl.pallas_call(
            _kernel,
            out_shape=[
                jax.ShapeDtypeStruct((OWN, D), bf16),
                jax.ShapeDtypeStruct((G, D, HEAD), bf16),
                jax.ShapeDtypeStruct((NC + 1, HEADS * HEAD, CW), bf16),
                jax.ShapeDtypeStruct((NC + 1, OWN, CW), f32),
                jax.ShapeDtypeStruct((ROWS, HEADS * HEAD), bf16),
                jax.ShapeDtypeStruct((ROWS, D), bf16),
            ],
            in_specs=[hbm, vmem, hbm, hbm, hbm, hbm, hbm],
            out_specs=[hbm] * 6,
            scratch_shapes=[
                pltpu.VMEM((TOK, D), bf16),
                pltpu.VMEM((2, 8 * OWN, HEAD), bf16),
                pltpu.VMEM((HEAD + 8, 8 * OWN), bf16),
                pltpu.VMEM((TOK, HEADS * HEAD), bf16),
                pltpu.VMEM((2, D, HEAD), bf16),
                pltpu.VMEM((TOK, HEAD), bf16),
                pltpu.VMEM((TOK, HEAD), f32),
                pltpu.VMEM((1, TOK), f32),
                pltpu.VMEM((HEAD + 8, TOK), f32),
                pltpu.VMEM((2, HEADS * HEAD, CW), bf16),
                pltpu.VMEM((4, TOK, CW), f32),
                pltpu.VMEM((2, OWN, CW), f32),
                pltpu.VMEM((2, OWN, CW // 2), f32),
                pltpu.VMEM((2, OWN, CW), bf16),
                pltpu.VMEM((2, OWN, CW), bf16),
                pltpu.VMEM((OWN + 8, HEAD), f32),
                *[pltpu.VMEM((TOK, HALF), f32)] * 2,
                pltpu.VMEM((1, D), f32),
                *(dma, dma((G, 2)), dma, dma((G,)), dma, dma((G, 2))),
                *(dma((4,)), dma((G, 3)), dma((2,)), dma((3,))),
                *[dma((PIECES,))] * 3,
                dma((7, 2)),
                dma((2, 8)),
                dma((2, 8)),
                *(dma, dma((NC + 2,)), dma, dma((NC + 2,))),
                dma((2, 4)),
                *(dma((4,)), dma((NC + 2,))),
                *[dma((2,))] * 3,
                dma,
            ],
            compiler_params=pltpu.CompilerParams(collective_id=0, has_side_effects=True, vmem_limit_bytes=VMEM),
            cost_estimate=pl.CostEstimate(flops=2 * 10**11, bytes_accessed=4 * 10**8, transcendentals=5 * 10**7),
        )(x, gain, wk, wv, wq, wo, jnp.asarray(turns))
        return out[0]

    tokens, whole = P(("dp", "sp"), None), P("sp", None)
    return jax.shard_map(
        step,
        mesh=mesh,
        in_specs=(tokens, P(None), whole, whole, whole, whole),
        out_specs=tokens,
        check_vma=False,
    )
```

```python
import jax
import jax.numpy as jnp
import numpy as np
from jax import lax
from jax.experimental import pallas as pl
from jax.experimental.pallas import tpu as pltpu
from jax.sharding import PartitionSpec as P

HEAD = 256
HALF = HEAD // 2
THETA = 10000
NEG = -1e30
HIDDEN = 2 * NEG
LOG2E = 1.4426950408889634
MESH = pl.DeviceIdType.MESH
D = 8192
OWN = 512
TOK = 2 * OWN
ROWS = 1024
HEADS = 16
G = HEADS + 1
CW = 256
NC = D // CW - 1
PIECE = 128
PIECES = OWN // PIECE
STRIP = 256
VMEM = 54 * 2**20


def _dot(a, b, ca=1, cb=0):
    return lax.dot_general(a, b, (((ca,), (cb,)), ((), ())), preferred_element_type=jnp.float32)


def _turn(t, cos, sin):
    a, b = t[:, :HALF], t[:, HALF:]
    return jnp.concatenate([a * cos - b * sin, b * cos + a * sin], axis=-1).astype(jnp.bfloat16)


def _kernel(x, gain, wk, wv, wq, wo, turns, y, WQ, WO, PR, SQ, SO,
            A, KV, VT, seen, wbuf, q_s, acc, top_s, mix_s, wob, obuf, prb, plast, xb, tab, cos, sin, gp,
            sn, rn, sm, rm, sf, rf, sd, rd, so, ro, sxp, rxp, lxp, sk, rk, wst, swm, rwm, swd, rwd, wos, sp, rp, prs, xcs, tabs):
    me = lax.axis_index("sp")
    j, i, c = lax.div(me, 4), lax.rem(lax.div(me, 2), 2), lax.rem(me, 2)
    sib, nb, mb = me + 1 - 2 * c, me + 4 - 8 * j, me + 2 - 4 * i

    def remote(src, dst, s, r, dev):
        return pltpu.make_async_remote_copy(src_ref=src, dst_ref=dst, send_sem=s, recv_sem=r, device_id={"sp": dev}, device_id_type=MESH)

    def local(src, dst, s):
        return pltpu.make_async_copy(src, dst, s)

    def rows(e):
        return pl.ds(pl.multiple_of(e * ROWS, ROWS), ROWS)

    def tokens(t):
        return pl.ds(pl.multiple_of(t * OWN, OWN), OWN)

    def qcols(jj, g):
        return pl.ds(pl.multiple_of(jj * (HEADS * HEAD) + (g - 1) * HEAD, HEAD), HEAD)

    def mate(b):
        b2, b1, b0 = b // 4, b // 2 % 2, b % 2
        return 4 * (j + b2 - 2 * j * b2) + 2 * (i + b1 - 2 * i * b1) + (c + b0 - 2 * c * b0)

    def half(e, k):
        return pl.ds(pl.multiple_of(e * ROWS + k * (ROWS // 2), ROWS // 2), ROWS // 2)

    def own_n(g):
        for k in range(2):
            src = wq.at[k * (ROWS // 2) : (k + 1) * (ROWS // 2), qcols(1 - j, g)]
            remote(src, WQ.at[g, half(me, k), :], sn, rn.at[g, k], nb).start()

    def own_m(g):
        return remote(wq.at[:, qcols(j, g)], WQ.at[g, rows(me), :], sm, rm.at[g], mb)

    def own_d():
        return remote(wq.at[:, pl.ds(pl.multiple_of(j * HEADS * HEAD, HEAD), HEADS * HEAD)], SQ, so.at[0], ro.at[0], sib)

    def wo_d():
        return remote(wo, SO, so.at[1], ro.at[1], sib)

    def moved(g, b, s, r, dev):
        here = WQ.at[g, rows(mate(b)), :]
        return remote(here, here, s, r, dev)

    def halved(g, b, k, s, r, dev):
        here = WQ.at[g, half(mate(b), k), :]
        return remote(here, here, s, r.at[g, k], dev)

    def relay_n(g, k):
        halved(g, 4, k, sn, rn, nb).wait_recv()
        halved(g, 4, k, sf, rf, mb).start()

    def pass_d(g, kind):
        return moved(g, {1: 4, 2: 2, 3: 6}[kind], sd.at[kind], rd.at[g, kind - 1], sib)

    def got_m(g):
        moved(g, 2, sm, rm.at[g], mb).wait_recv()

    def got_f(g):
        for k in range(2):
            halved(g, 6, k, sf, rf, mb).wait_recv()

    def got_d(g, kind):
        moved(g, {1: 5, 2: 3, 3: 7}[kind], sd.at[kind], rd.at[g, kind - 1], sib).wait_recv()

    def stage(g, b):
        slot = lax.rem(g, 2)
        return local(WQ.at[g, rows(mate(b)), :], wbuf.at[slot, b * ROWS : (b + 1) * ROWS, :], wst.at[slot, b])

    def stage_early(g):
        slot = lax.rem(g, 2)
        local(wq.at[:, qcols(j, g)], wbuf.at[slot, :ROWS, :], wst.at[slot, 0]).start()
        local(SQ.at[:, pl.ds(pl.multiple_of((g - 1) * HEAD, HEAD), HEAD)], wbuf.at[slot, ROWS : 2 * ROWS, :], wst.at[slot, 1]).start()
        stage(g, 2).start()
        got_d(g, 2)
        stage(g, 3).start()

    def block(n):
        return n, n, 0, CW

    tail = [(NC + k, NC, k * CW // 2, CW // 2) for k in range(2)]

    def wo_here(n, at, off, w):
        return wo.at[:, pl.ds(pl.multiple_of(at * CW + off, 128), w)]

    def wo_there(owner, n, at, off, w):
        return WO.at[at, rows(owner), off : off + w]

    def wo_m(k):
        return remote(wo_here(*k), wo_there(2 * i + c, *k), swm, rwm.at[k[0]], mb)

    def wo_pass(k):
        part = wo_there(2 * (1 - i) + c, *k)
        return remote(part, part, swd, rwd.at[k[0]], sib)

    def kv_block(kv, t, s, dev):
        return remote(KV.at[kv, tokens(t), :], KV.at[kv, tokens(t), :], s, rk.at[kv, t], dev)

    def piece(p):
        return pl.ds(pl.multiple_of(p * PIECE, PIECE), PIECE)


    def x_send(p):
        for b in range(8):
            remote(x.at[pl.ds(p * PIECE, PIECE), rows(mate(b ^ 4))], A.at[piece(p), b * ROWS : (b + 1) * ROWS], sxp.at[p], rxp.at[p], nb).start()

    def x_whole(p):
        return remote(A.at[piece(p), :], A.at[piece(p), :], sxp.at[p], rxp.at[p], nb)

    barrier = pltpu.get_barrier_semaphore()
    for dev in (sib, nb, mb):
        pl.semaphore_signal(barrier, inc=1, device_id={"sp": dev}, device_id_type=MESH)
    pl.semaphore_wait(barrier, 3)

    def first_blocks(mine, other):
        for k in range(2):
            remote(other.at[k * (ROWS // 2) : (k + 1) * (ROWS // 2), :], WQ.at[0, half(me, k), :], sn, rn.at[0, k], nb).start()
        remote(mine, WQ.at[0, rows(me), :], sm, rm.at[0], mb).start()
        remote(mine, WQ.at[0, rows(me), :], sd.at[0], ro.at[2], sib).start()
        local(mine, wbuf.at[0, :ROWS, :], wst.at[0, 0]).start()

    @pl.when(j == 0)
    def _():
        first_blocks(wk, wv)

    @pl.when(j == 1)
    def _():
        first_blocks(wv, wk)

    x_send(0)
    x_send(1)
    own_m(1).start()
    for p in range(PIECES):
        for b in range(8):
            local(x.at[pl.ds(p * PIECE, PIECE), rows(mate(b))], y.at[piece(p), b * ROWS : (b + 1) * ROWS], lxp.at[p]).start()
    local(turns, tab, tabs).start()

    own_d().start()

    for b in range(8):
        gp[:, b * ROWS : (b + 1) * ROWS] = gain[rows(mate(b))].astype(jnp.float32).reshape(1, ROWS)

    local(turns, tab, tabs).wait()
    for jj in range(2):
        here = lax.broadcasted_iota(jnp.int32, (8, HEAD), 0) == 4 * jj + 2 * i + c
        turn = jnp.sum(jnp.where(here, tab[OWN:, :], 0.0), axis=0, keepdims=True)
        cr, sr, ct, st = tab[:OWN, :HALF], tab[:OWN, HALF:], turn[:, :HALF], turn[:, HALF:]
        cos[jj * OWN : (jj + 1) * OWN, :] = cr * ct - sr * st
        sin[jj * OWN : (jj + 1) * OWN, :] = sr * ct + cr * st

    relay_n(0, 0)
    relay_n(0, 1)
    pass_d(0, 1).start()
    stage(0, 4).start()

    @pl.loop(2, 6)
    def _(g):
        own_m(g).start()

    got_m(0)
    pass_d(0, 2).start()
    stage(0, 2).start()
    got_f(0)
    pass_d(0, 3).start()
    stage(0, 6).start()
    moved(0, 1, sd.at[0], ro.at[2], sib).wait_recv()
    stage(0, 1).start()
    for kind, b in ((2, 3), (1, 5), (3, 7)):
        got_d(0, kind)
        stage(0, b).start()
    for b in range(8):
        stage(0, b).wait()

    def norm_and_kv(p, jj, a):
        at = pl.multiple_of(p * PIECE, PIECE)

        @pl.loop(0, PIECE // 16)
        def _(r):
            here = pl.ds(pl.multiple_of(at + r * 16, 16), 16)
            wide = a[here, :].astype(jnp.float32)
            scale = lax.rsqrt(jnp.mean(wide * wide, -1, keepdims=True) + 1e-6)
            a[here, :] = (wide * scale * gp[...]).astype(jnp.bfloat16)

        t = _dot(a[pl.ds(at, PIECE), :], wbuf[0]).astype(jnp.bfloat16)
        here = pl.ds(pl.multiple_of(jj * OWN + p * PIECE, PIECE), PIECE)
        turned = _turn(t.astype(jnp.float32), cos[here, :], sin[here, :])
        first = pl.multiple_of((4 * jj + 2 * i + c) * OWN + p * PIECE, PIECE)
        KV[j, pl.ds(first, PIECE), :] = jnp.where(j == 0, turned, t)

    def kv_send(t, which):
        for k, dev in enumerate((nb, mb, sib)):
            kv_block(j, t, sk.at[k, which], dev).start()

    def kv_pass(t, which):
        kv_block(j, t, sk.at[3, which], mb).wait_recv()
        kv_block(j, t, sk.at[3, which], nb).start()
        kv_block(j, t, sk.at[4, which], sib).start()

    def relay(g):
        got_m(g)
        pass_d(g, 2).start()

    for p in range(PIECES):
        local(y.at[piece(p), :], y.at[piece(p), :], lxp.at[p]).wait()

    @pl.loop(0, PIECES)
    def _(p):
        norm_and_kv(p, j, y)

    kv_send(me, 0)
    x_send(2)

    wo_d().start()

    @pl.loop(6, G)
    def _(g):
        own_m(g).start()

    @pl.loop(0, PIECES)
    def _(p):
        @pl.when(p == 2)
        def _():
            kv_pass(mb, 0)
            x_send(3)
            own_n(1)

        @pl.loop(3 * p + 1, 3 * p + 4)
        def _(g):
            relay(g)

        x_whole(p).wait_recv()
        norm_and_kv(p, 1 - j, A)

    kv_send(nb, 1)
    wo_m(block(0)).start()
    kv_pass(mate(6), 1)
    own_n(2)
    own_n(3)

    @pl.loop(3 * PIECES + 1, G)
    def _(g):
        relay(g)

    own_d().wait_recv()
    wo_d().wait_recv()
    relay_n(1, 0)
    relay_n(1, 1)
    pass_d(1, 1).start()
    stage_early(1)

    for which, b in enumerate((4, 6, 0, 2)):
        kv_block(1 - j, mate(b), sk.at[5, which % 2], nb).wait_recv()
        kv_block(1 - j, mate(b), sk.at[5 + which // 2, which % 2], sib).start()
    for kv in range(2):
        for b in (1, 3, 5, 7):
            kv_block(kv, mate(b), sk.at[6, 0], sib).wait_recv()

    relay_n(2, 0)

    @pl.loop(0, 8)
    def _(t):
        VT[:HEAD, tokens(t)] = KV[1, tokens(t), :].T
        VT[HEAD:, tokens(t)] = jnp.ones((8, OWN), jnp.bfloat16)

    e2 = HEAD**-0.5 * LOG2E
    low = 2 * i + c

    def step(work):
        scores = [_dot(KV[0, pl.ds(key, n), :], q_s[at : at + STRIP, :], 1, 1) for at, key, n, _ in work]
        weights, keeps = [], []
        for (at, key, n, cut), s in zip(work, scores):
            if cut:
                gap = lax.broadcasted_iota(jnp.int32, (OWN, STRIP), 1) + at % OWN - lax.broadcasted_iota(jnp.int32, (OWN, STRIP), 0)
                last = jnp.where(gap >= 0, s[n - OWN :], HIDDEN)
                s = last if n == OWN else jnp.concatenate([s[: n - OWN], last], axis=0)
            old = top_s[:, at : at + STRIP]
            top = jnp.maximum(old, s.max(axis=0, keepdims=True))
            top_s[:, at : at + STRIP] = top
            weights.append(jnp.exp2((s - top) * e2).astype(jnp.bfloat16))
            keeps.append(jnp.exp2((old - top) * e2))
        for (at, key, n, _), p, keep in zip(work, weights, keeps):
            mix_s[:, at : at + STRIP] = mix_s[:, at : at + STRIP] * keep + _dot(VT[:, pl.ds(key, n)], p)

    first, second = range(0, OWN, STRIP), range(OWN, TOK, STRIP)

    def attend(g):
        top_s[...] = jnp.full((1, TOK), NEG, jnp.float32)
        mix_s[...] = jnp.zeros((HEAD + 8, TOK), jnp.float32)

        @pl.loop(0, low)
        def _(t):
            key = pl.multiple_of(t * OWN, OWN)
            step([(at, key, OWN, False) for at in (*first, *second)])

        @pl.when(g + 2 < G)
        def _():
            relay_n(g + 2, 0)

        key = pl.multiple_of(low * OWN, OWN)
        step([(at, key, OWN, True) for at in first] + [(at, key, 2 * OWN, False) for at in second])
        key = pl.multiple_of((low + 2) * OWN, OWN)
        step([(at, key, 3 * OWN, True) for at in second])
        cols = pl.ds(pl.multiple_of((g - 1) * HEAD, HEAD), HEAD)
        for at in (*first, *second):
            total = mix_s[HEAD : HEAD + 1, at : at + STRIP]
            seen[at : at + STRIP, cols] = (mix_s[:HEAD, at : at + STRIP] * (1 / total)).T.astype(jnp.bfloat16)

    halves = [slice(0, OWN), slice(OWN, TOK)]

    own_rows = pl.ds(pl.multiple_of(j * OWN, OWN), OWN)
    mate_rows = pl.ds(pl.multiple_of((1 - j) * OWN, OWN), OWN)
    owners = [2 * i + c, 2 * i + 1 - c, 2 * (1 - i) + c, 2 * (1 - i) + 1 - c]

    def ring(n, size):
        return n % size if isinstance(n, int) else lax.rem(n, size)

    def ocols(n, at, off, w):
        return pl.ds(pl.multiple_of(at * CW + off, 128), w)

    def part_copy(k):
        n, at, off, w = k
        dst = PR.at[at] if w == CW else plast.at[n - NC]
        return remote(obuf.at[ring(n, 4), mate_rows, :w], dst, sp.at[ring(n, 4)], rp.at[n], nb)

    def part_in(k):
        n, at, _, _ = k
        return local(PR.at[at], prb.at[ring(n, 2)], prs.at[ring(n, 2)])

    def x_in(k):
        return local(x.at[:, ocols(*k)], xb.at[ring(k[0], 2), :, : k[3]], xcs.at[ring(k[0], 2)])

    def ostage(k, o):
        src = wo_here(*k) if o == 0 else SO.at[:, ocols(*k)] if o == 1 else wo_there(owners[o], *k)
        return local(src, wob.at[ring(k[0], 2), rows(owners[o]), : k[3]], wos.at[ring(k[0], 2), o])

    def wo_got(k, o):
        part = wo_there(owners[o], *k)
        s, r, dev = (swm, rwm.at[k[0]], mb) if o == 2 else (swd, rwd.at[k[0]], sib)
        remote(part, part, s, r, dev).wait_recv()

    def finish(k):
        n, _, _, w = k
        slot = ring(n, 2)
        x_in(k).start()
        part_copy(k).wait_recv()
        if w == CW:
            part_in(k).start()
            part_in(k).wait()
        x_in(k).wait()
        part = prb[slot] if w == CW else plast[n - NC]
        y[:, ocols(*k)] = (xb[slot, :, :w].astype(jnp.float32) + (obuf[ring(n, 4), own_rows, :w] + part)).astype(jnp.bfloat16)

    def share(k):
        wo_got(k, 2)
        wo_pass(k).start()

    def fetch(k):
        ostage(k, 0).start()
        ostage(k, 1).start()
        if not isinstance(k[0], int) or k[0] > 0:
            share(k)
        ostage(k, 2).start()
        wo_got(k, 3)
        ostage(k, 3).start()

    def multiply(k):
        n, _, _, w = k
        slot = ring(n, 2)
        for o in range(4):
            ostage(k, o).wait()
        if w == CW:
            obuf[ring(n, 4)] = _dot(seen[...], wob[slot])
        else:
            for r in halves:
                obuf[ring(n, 4), r, :w] = _dot(seen[r, :], wob[slot, :, :w])
        part_copy(k).start()

    @pl.loop(1, G)
    def _(g):
        @pl.when(g + 3 < G)
        def _():
            own_n(g + 3)

        got_f(g)
        pass_d(g, 3).start()
        stage(g, 6).start()
        stage(g, 4).start()
        got_d(g, 1)
        stage(g, 5).start()
        slot = lax.rem(g, 2)

        for b in range(4):
            stage(g, b).wait()
        for r, a in zip(halves, (y, A)):
            acc[r, :] = _dot(a[:, : 4 * ROWS], wbuf[slot, : 4 * ROWS, :])

        @pl.when(g + 1 < G)
        def _():
            relay_n(g + 1, 1)
            pass_d(g + 1, 1).start()

        @pl.when(g == G - 2)
        def _():
            @pl.loop(1, NC)
            def _(n):
                wo_m(block(n)).start()

            for k in tail:
                wo_m(k).start()

        got_d(g, 3)
        stage(g, 7).start()
        stage(g, 4).wait()
        stage(g, 5).wait()
        for r, a in zip(halves, (y, A)):
            acc[r, :] += _dot(a[:, 4 * ROWS : 6 * ROWS], wbuf[slot, 4 * ROWS : 6 * ROWS, :])
        stage(g, 6).wait()
        stage(g, 7).wait()
        for r, a, to in zip(halves, (y, A), (own_rows, mate_rows)):
            t = acc[r, :] + _dot(a[:, 6 * ROWS :], wbuf[slot, 6 * ROWS :, :])
            q_s[to, :] = _turn(t.astype(jnp.bfloat16).astype(jnp.float32), cos[to, :], sin[to, :])

        @pl.when(g + 1 < G)
        def _():
            stage_early(g + 1)

        @pl.when(g == HEADS // 2)
        def _():
            share(block(0))

        @pl.when(g == G - 1)
        def _():
            fetch(block(0))

        attend(g)

    @pl.loop(0, NC)
    def _(n):
        @pl.when(n >= 4)
        def _():
            part_copy(block(n - 4)).wait_send()

        @pl.when(n > 0)
        def _():
            fetch(block(n))

        multiply(block(n))

        @pl.when(n >= 2)
        def _():
            finish(block(n - 2))

    late = [block(n) for n in range(NC - 4, NC)] + tail
    for m in (4, 5):
        part_copy(late[m - 4]).wait_send()
        fetch(late[m])
        multiply(late[m])
        finish(late[m - 2])
    for m in (4, 5):
        finish(late[m])
    for m in (2, 3, 4, 5):
        part_copy(late[m]).wait_send()

    sent = WQ.at[:, rows(0), :]
    for k, dev in ((sn, nb), (sm, mb), (sf, mb), (sd.at[1], sib), (sd.at[2], sib), (sd.at[3], sib)):
        remote(sent, sent, k, rm.at[0], dev).wait_send()
    moved(0, 0, sd.at[0], rm.at[0], sib).wait_send()
    own_d().wait_send()
    wo_d().wait_send()
    sent = WO.at[:, rows(0), :]
    for k, dev in ((swm, mb), (swd, sib)):
        remote(sent, sent, k, rm.at[0], dev).wait_send()
    for p in range(PIECES):
        x_whole(p).wait_send()
    for k, dev in enumerate((nb, mb, sib, nb, sib, sib, sib)):
        for which in range(2):
            kv_block(0, 0, sk.at[k, which], dev).wait_send()


def solution(mesh):
    def step(x, gain, wq, wk, wv, wo):
        rate = THETA ** (-np.arange(HALF) / HALF)
        angle = np.concatenate([np.arange(OWN), OWN * np.arange(8)])[:, None] * rate
        turns = np.concatenate([np.cos(angle), np.sin(angle)], axis=1).astype(np.float32)
        bf16, f32, dma = jnp.bfloat16, jnp.float32, pltpu.SemaphoreType.DMA
        hbm, vmem = pl.BlockSpec(memory_space=pltpu.HBM), pl.BlockSpec(memory_space=pltpu.VMEM)
        out = pl.pallas_call(
            _kernel,
            out_shape=[
                pltpu.VMEM((OWN, D), bf16),
                jax.ShapeDtypeStruct((G, D, HEAD), bf16),
                jax.ShapeDtypeStruct((NC + 1, HEADS * HEAD, CW), bf16),
                jax.ShapeDtypeStruct((NC + 1, OWN, CW), f32),
                jax.ShapeDtypeStruct((ROWS, HEADS * HEAD), bf16),
                jax.ShapeDtypeStruct((ROWS, D), bf16),
            ],
            in_specs=[hbm, vmem, hbm, hbm, hbm, hbm, hbm],
            out_specs=[pl.BlockSpec(memory_space=pltpu.VMEM)] + [hbm] * 5,
            scratch_shapes=[
                pltpu.VMEM((OWN, D), bf16),
                pltpu.VMEM((2, 8 * OWN, HEAD), bf16),
                pltpu.VMEM((HEAD + 8, 8 * OWN), bf16),
                pltpu.VMEM((TOK, HEADS * HEAD), bf16),
                pltpu.VMEM((2, D, HEAD), bf16),
                pltpu.VMEM((TOK, HEAD), bf16),
                pltpu.VMEM((TOK, HEAD), f32),
                pltpu.VMEM((1, TOK), f32),
                pltpu.VMEM((HEAD + 8, TOK), f32),
                pltpu.VMEM((2, HEADS * HEAD, CW), bf16),
                pltpu.VMEM((4, TOK, CW), f32),
                pltpu.VMEM((2, OWN, CW), f32),
                pltpu.VMEM((2, OWN, CW // 2), f32),
                pltpu.VMEM((2, OWN, CW), bf16),
                pltpu.VMEM((OWN + 8, HEAD), f32),
                *[pltpu.VMEM((TOK, HALF), f32)] * 2,
                pltpu.VMEM((1, D), f32),
                *(dma, dma((G, 2)), dma, dma((G,)), dma, dma((G, 2))),
                *(dma((4,)), dma((G, 3)), dma((2,)), dma((3,))),
                *[dma((PIECES,))] * 3,
                dma((7, 2)),
                dma((2, 8)),
                dma((2, 8)),
                *(dma, dma((NC + 2,)), dma, dma((NC + 2,))),
                dma((2, 4)),
                *(dma((4,)), dma((NC + 2,))),
                *[dma((2,))] * 2,
                dma,
            ],
            compiler_params=pltpu.CompilerParams(collective_id=0, has_side_effects=True, vmem_limit_bytes=VMEM),
            cost_estimate=pl.CostEstimate(flops=2 * 10**11, bytes_accessed=4 * 10**8, transcendentals=5 * 10**7),
        )(x, gain, wk, wv, wq, wo, jnp.asarray(turns))
        return out[0]

    tokens, whole = P(("dp", "sp"), None), P("sp", None)
    return jax.shard_map(
        step,
        mesh=mesh,
        in_specs=(tokens, P(None), whole, whole, whole, whole),
        out_specs=tokens,
        check_vma=False,
    )
```

```python
import jax
import jax.numpy as jnp
import numpy as np
from jax import lax
from jax.experimental import pallas as pl
from jax.experimental.pallas import tpu as pltpu
from jax.sharding import PartitionSpec as P

HEAD = 256
HALF = HEAD // 2
THETA = 10000
NEG = -1e30
HIDDEN = 2 * NEG
LOG2E = 1.4426950408889634
MESH = pl.DeviceIdType.MESH
D = 8192
OWN = 512
TOK = 2 * OWN
ROWS = 1024
HEADS = 16
G = HEADS + 1
CW = 256
NC = D // CW - 1
PIECE = 128
PIECES = OWN // PIECE
STRIP = 256
VMEM = 54 * 2**20


def _dot(a, b, ca=1, cb=0):
    return lax.dot_general(a, b, (((ca,), (cb,)), ((), ())), preferred_element_type=jnp.float32)


def _turn(t, cos, sin):
    a, b = t[:, :HALF], t[:, HALF:]
    return jnp.concatenate([a * cos - b * sin, b * cos + a * sin], axis=-1).astype(jnp.bfloat16)


def _kernel(x, gain, wk, wv, wq, wo, turns, y, WQ, WO, PR, SQ, SO,
            A, KV, VT, seen, wbuf, q_s, acc, top_s, mix_s, wob, obuf, prb, plast, xb, tab, cos, sin, gp,
            sn, rn, sm, rm, sf, rf, sd, rd, so, ro, sxp, rxp, lxp, sk, rk, wst, swm, rwm, swd, rwd, wos, sp, rp, prs, xcs, tabs):
    me = lax.axis_index("sp")
    j, i, c = lax.div(me, 4), lax.rem(lax.div(me, 2), 2), lax.rem(me, 2)
    sib, nb, mb = me + 1 - 2 * c, me + 4 - 8 * j, me + 2 - 4 * i

    def remote(src, dst, s, r, dev):
        return pltpu.make_async_remote_copy(src_ref=src, dst_ref=dst, send_sem=s, recv_sem=r, device_id={"sp": dev}, device_id_type=MESH)

    def local(src, dst, s):
        return pltpu.make_async_copy(src, dst, s)

    def rows(e):
        return pl.ds(pl.multiple_of(e * ROWS, ROWS), ROWS)

    def tokens(t):
        return pl.ds(pl.multiple_of(t * OWN, OWN), OWN)

    def qcols(jj, g):
        return pl.ds(pl.multiple_of(jj * (HEADS * HEAD) + (g - 1) * HEAD, HEAD), HEAD)

    def mate(b):
        b2, b1, b0 = b // 4, b // 2 % 2, b % 2
        return 4 * (j + b2 - 2 * j * b2) + 2 * (i + b1 - 2 * i * b1) + (c + b0 - 2 * c * b0)

    def half(e, k):
        return pl.ds(pl.multiple_of(e * ROWS + k * (ROWS // 2), ROWS // 2), ROWS // 2)

    def own_n(g):
        for k in range(2):
            src = wq.at[k * (ROWS // 2) : (k + 1) * (ROWS // 2), qcols(1 - j, g)]
            remote(src, WQ.at[g, half(me, k), :], sn, rn.at[g, k], nb).start()

    def own_m(g):
        return remote(wq.at[:, qcols(j, g)], WQ.at[g, rows(me), :], sm, rm.at[g], mb)

    def own_d():
        return remote(wq.at[:, pl.ds(pl.multiple_of(j * HEADS * HEAD, HEAD), HEADS * HEAD)], SQ, so.at[0], ro.at[0], sib)

    def wo_d():
        return remote(wo, SO, so.at[1], ro.at[1], sib)

    def moved(g, b, s, r, dev):
        here = WQ.at[g, rows(mate(b)), :]
        return remote(here, here, s, r, dev)

    def halved(g, b, k, s, r, dev):
        here = WQ.at[g, half(mate(b), k), :]
        return remote(here, here, s, r.at[g, k], dev)

    def relay_n(g, k):
        halved(g, 4, k, sn, rn, nb).wait_recv()
        halved(g, 4, k, sf, rf, mb).start()

    def pass_d(g, kind):
        return moved(g, {1: 4, 2: 2, 3: 6}[kind], sd.at[kind], rd.at[g, kind - 1], sib)

    def got_m(g):
        moved(g, 2, sm, rm.at[g], mb).wait_recv()

    def got_f(g):
        for k in range(2):
            halved(g, 6, k, sf, rf, mb).wait_recv()

    def got_d(g, kind):
        moved(g, {1: 5, 2: 3, 3: 7}[kind], sd.at[kind], rd.at[g, kind - 1], sib).wait_recv()

    def stage(g, b):
        slot = lax.rem(g, 2)
        return local(WQ.at[g, rows(mate(b)), :], wbuf.at[slot, b * ROWS : (b + 1) * ROWS, :], wst.at[slot, b])

    def stage_early(g):
        slot = lax.rem(g, 2)
        local(wq.at[:, qcols(j, g)], wbuf.at[slot, :ROWS, :], wst.at[slot, 0]).start()
        local(SQ.at[:, pl.ds(pl.multiple_of((g - 1) * HEAD, HEAD), HEAD)], wbuf.at[slot, ROWS : 2 * ROWS, :], wst.at[slot, 1]).start()
        stage(g, 2).start()
        got_d(g, 2)
        stage(g, 3).start()

    def block(n):
        return n, n - 1, 0, CW

    head = [(k, 0, k * CW // 2, CW // 2) for k in range(2)]
    tail = [(NC + 1 + k, NC, k * CW // 2, CW // 2) for k in range(2)]

    def wo_here(n, at, off, w):
        return wo.at[:, pl.ds(pl.multiple_of(at * CW + off, 128), w)]

    def wo_there(owner, n, at, off, w):
        return WO.at[at, rows(owner), off : off + w]

    def wo_m(k):
        return remote(wo_here(*k), wo_there(2 * i + c, *k), swm, rwm.at[k[0]], mb)

    def wo_pass(k):
        part = wo_there(2 * (1 - i) + c, *k)
        return remote(part, part, swd, rwd.at[k[0]], sib)

    def kv_block(kv, t, s, dev):
        return remote(KV.at[kv, tokens(t), :], KV.at[kv, tokens(t), :], s, rk.at[kv, t], dev)

    def piece(p):
        return pl.ds(pl.multiple_of(p * PIECE, PIECE), PIECE)


    def x_send(p):
        for b in range(8):
            remote(x.at[pl.ds(p * PIECE, PIECE), rows(mate(b ^ 4))], A.at[piece(p), b * ROWS : (b + 1) * ROWS], sxp.at[p], rxp.at[p], nb).start()

    def x_whole(p):
        return remote(A.at[piece(p), :], A.at[piece(p), :], sxp.at[p], rxp.at[p], nb)

    barrier = pltpu.get_barrier_semaphore()
    for dev in (sib, nb, mb):
        pl.semaphore_signal(barrier, inc=1, device_id={"sp": dev}, device_id_type=MESH)
    pl.semaphore_wait(barrier, 3)

    def first_blocks(mine, other):
        for k in range(2):
            remote(other.at[k * (ROWS // 2) : (k + 1) * (ROWS // 2), :], WQ.at[0, half(me, k), :], sn, rn.at[0, k], nb).start()
        remote(mine, WQ.at[0, rows(me), :], sm, rm.at[0], mb).start()
        remote(mine, WQ.at[0, rows(me), :], sd.at[0], ro.at[2], sib).start()
        local(mine, wbuf.at[0, :ROWS, :], wst.at[0, 0]).start()

    @pl.when(j == 0)
    def _():
        first_blocks(wk, wv)

    @pl.when(j == 1)
    def _():
        first_blocks(wv, wk)

    x_send(0)
    x_send(1)
    own_m(1).start()
    for p in range(PIECES):
        for b in range(8):
            local(x.at[pl.ds(p * PIECE, PIECE), rows(mate(b))], y.at[piece(p), b * ROWS : (b + 1) * ROWS], lxp.at[p]).start()
    local(turns, tab, tabs).start()

    own_d().start()

    for b in range(8):
        gp[:, b * ROWS : (b + 1) * ROWS] = gain[rows(mate(b))].astype(jnp.float32).reshape(1, ROWS)

    local(turns, tab, tabs).wait()
    for jj in range(2):
        here = lax.broadcasted_iota(jnp.int32, (8, HEAD), 0) == 4 * jj + 2 * i + c
        turn = jnp.sum(jnp.where(here, tab[OWN:, :], 0.0), axis=0, keepdims=True)
        cr, sr, ct, st = tab[:OWN, :HALF], tab[:OWN, HALF:], turn[:, :HALF], turn[:, HALF:]
        cos[jj * OWN : (jj + 1) * OWN, :] = cr * ct - sr * st
        sin[jj * OWN : (jj + 1) * OWN, :] = sr * ct + cr * st

    relay_n(0, 0)
    relay_n(0, 1)
    pass_d(0, 1).start()
    stage(0, 4).start()

    @pl.loop(2, 6)
    def _(g):
        own_m(g).start()

    got_m(0)
    pass_d(0, 2).start()
    stage(0, 2).start()
    got_f(0)
    pass_d(0, 3).start()
    stage(0, 6).start()
    moved(0, 1, sd.at[0], ro.at[2], sib).wait_recv()
    stage(0, 1).start()
    for kind, b in ((2, 3), (1, 5), (3, 7)):
        got_d(0, kind)
        stage(0, b).start()
    for b in range(8):
        stage(0, b).wait()

    def norm_and_kv(p, jj, a):
        at = pl.multiple_of(p * PIECE, PIECE)

        @pl.loop(0, PIECE // 16)
        def _(r):
            here = pl.ds(pl.multiple_of(at + r * 16, 16), 16)
            wide = a[here, :].astype(jnp.float32)
            scale = lax.rsqrt(jnp.mean(wide * wide, -1, keepdims=True) + 1e-6)
            a[here, :] = (wide * scale * gp[...]).astype(jnp.bfloat16)

        t = _dot(a[pl.ds(at, PIECE), :], wbuf[0]).astype(jnp.bfloat16)
        here = pl.ds(pl.multiple_of(jj * OWN + p * PIECE, PIECE), PIECE)
        turned = _turn(t.astype(jnp.float32), cos[here, :], sin[here, :])
        first = pl.multiple_of((4 * jj + 2 * i + c) * OWN + p * PIECE, PIECE)
        KV[j, pl.ds(first, PIECE), :] = jnp.where(j == 0, turned, t)

    def kv_send(t, which):
        for k, dev in enumerate((nb, mb, sib)):
            kv_block(j, t, sk.at[k, which], dev).start()

    def kv_pass(t, which):
        kv_block(j, t, sk.at[3, which], mb).wait_recv()
        kv_block(j, t, sk.at[3, which], nb).start()
        kv_block(j, t, sk.at[4, which], sib).start()

    def relay(g):
        got_m(g)
        pass_d(g, 2).start()

    for p in range(PIECES):
        local(y.at[piece(p), :], y.at[piece(p), :], lxp.at[p]).wait()

    @pl.loop(0, PIECES)
    def _(p):
        norm_and_kv(p, j, y)

    kv_send(me, 0)
    x_send(2)

    wo_d().start()

    @pl.loop(6, G)
    def _(g):
        own_m(g).start()

    @pl.loop(0, PIECES)
    def _(p):
        @pl.when(p == 2)
        def _():
            kv_pass(mb, 0)
            x_send(3)
            own_n(1)

        @pl.loop(3 * p + 1, 3 * p + 4)
        def _(g):
            relay(g)

        x_whole(p).wait_recv()
        norm_and_kv(p, 1 - j, A)

    kv_send(nb, 1)
    wo_m(head[0]).start()
    kv_pass(mate(6), 1)
    own_n(2)
    own_n(3)

    @pl.loop(3 * PIECES + 1, G)
    def _(g):
        relay(g)

    own_d().wait_recv()
    wo_d().wait_recv()
    relay_n(1, 0)
    relay_n(1, 1)
    pass_d(1, 1).start()
    stage_early(1)

    for which, b in enumerate((4, 6, 0, 2)):
        kv_block(1 - j, mate(b), sk.at[5, which % 2], nb).wait_recv()
        kv_block(1 - j, mate(b), sk.at[5 + which // 2, which % 2], sib).start()
    for kv in range(2):
        for b in (1, 3, 5, 7):
            kv_block(kv, mate(b), sk.at[6, 0], sib).wait_recv()

    relay_n(2, 0)

    @pl.loop(0, 8)
    def _(t):
        VT[:HEAD, tokens(t)] = KV[1, tokens(t), :].T
        VT[HEAD:, tokens(t)] = jnp.ones((8, OWN), jnp.bfloat16)

    e2 = HEAD**-0.5 * LOG2E
    low = 2 * i + c

    def step(work):
        scores = [_dot(KV[0, pl.ds(key, n), :], q_s[at : at + STRIP, :], 1, 1) for at, key, n, _ in work]
        weights, keeps = [], []
        for (at, key, n, cut), s in zip(work, scores):
            if cut:
                gap = lax.broadcasted_iota(jnp.int32, (OWN, STRIP), 1) + at % OWN - lax.broadcasted_iota(jnp.int32, (OWN, STRIP), 0)
                last = jnp.where(gap >= 0, s[n - OWN :], HIDDEN)
                s = last if n == OWN else jnp.concatenate([s[: n - OWN], last], axis=0)
            old = top_s[:, at : at + STRIP]
            top = jnp.maximum(old, s.max(axis=0, keepdims=True))
            top_s[:, at : at + STRIP] = top
            weights.append(jnp.exp2((s - top) * e2).astype(jnp.bfloat16))
            keeps.append(jnp.exp2((old - top) * e2))
        for (at, key, n, _), p, keep in zip(work, weights, keeps):
            mix_s[:, at : at + STRIP] = mix_s[:, at : at + STRIP] * keep + _dot(VT[:, pl.ds(key, n)], p)

    first, second = range(0, OWN, STRIP), range(OWN, TOK, STRIP)

    def attend(g):
        top_s[...] = jnp.full((1, TOK), NEG, jnp.float32)
        mix_s[...] = jnp.zeros((HEAD + 8, TOK), jnp.float32)

        @pl.loop(0, low)
        def _(t):
            key = pl.multiple_of(t * OWN, OWN)
            step([(at, key, OWN, False) for at in (*first, *second)])

        @pl.when(g + 2 < G)
        def _():
            relay_n(g + 2, 0)

        key = pl.multiple_of(low * OWN, OWN)
        step([(at, key, OWN, True) for at in first] + [(at, key, 2 * OWN, False) for at in second])
        key = pl.multiple_of((low + 2) * OWN, OWN)
        step([(at, key, 3 * OWN, True) for at in second])
        cols = pl.ds(pl.multiple_of((g - 1) * HEAD, HEAD), HEAD)
        for at in (*first, *second):
            total = mix_s[HEAD : HEAD + 1, at : at + STRIP]
            seen[at : at + STRIP, cols] = (mix_s[:HEAD, at : at + STRIP] * (1 / total)).T.astype(jnp.bfloat16)

    halves = [slice(0, OWN), slice(OWN, TOK)]

    own_rows = pl.ds(pl.multiple_of(j * OWN, OWN), OWN)
    mate_rows = pl.ds(pl.multiple_of((1 - j) * OWN, OWN), OWN)
    owners = [2 * i + c, 2 * i + 1 - c, 2 * (1 - i) + c, 2 * (1 - i) + 1 - c]

    def ring(n, size):
        return n % size if isinstance(n, int) else lax.rem(n, size)

    def ocols(n, at, off, w):
        return pl.ds(pl.multiple_of(at * CW + off, 128), w)

    def part_copy(k):
        n, at, off, w = k
        dst = plast.at[n - NC - 1] if at is NC else PR.at[at, :, off : off + w]
        return remote(obuf.at[ring(n, 4), mate_rows, :w], dst, sp.at[ring(n, 4)], rp.at[n], nb)

    def part_in(k):
        n, at, off, w = k
        return local(PR.at[at, :, off : off + w], prb.at[ring(n, 2), :, :w], prs.at[ring(n, 2)])

    def x_in(k):
        return local(x.at[:, ocols(*k)], xb.at[ring(k[0], 2), :, : k[3]], xcs.at[ring(k[0], 2)])

    def ostage(k, o):
        src = wo_here(*k) if o == 0 else SO.at[:, ocols(*k)] if o == 1 else wo_there(owners[o], *k)
        return local(src, wob.at[ring(k[0], 2), rows(owners[o]), : k[3]], wos.at[ring(k[0], 2), o])

    def wo_got(k, o):
        part = wo_there(owners[o], *k)
        s, r, dev = (swm, rwm.at[k[0]], mb) if o == 2 else (swd, rwd.at[k[0]], sib)
        remote(part, part, s, r, dev).wait_recv()

    def finish(k):
        n, at, _, w = k
        slot = ring(n, 2)
        x_in(k).start()
        part_copy(k).wait_recv()
        if at is not NC:
            part_in(k).start()
            part_in(k).wait()
        x_in(k).wait()
        part = plast[n - NC - 1] if at is NC else prb[slot, :, :w]
        y[:, ocols(*k)] = (xb[slot, :, :w].astype(jnp.float32) + (obuf[ring(n, 4), own_rows, :w] + part)).astype(jnp.bfloat16)

    def share(k):
        wo_got(k, 2)
        wo_pass(k).start()

    def fetch(k):
        ostage(k, 0).start()
        ostage(k, 1).start()
        if not isinstance(k[0], int) or k[0] > 0:
            share(k)
        ostage(k, 2).start()
        wo_got(k, 3)
        ostage(k, 3).start()

    def multiply(k):
        n, _, _, w = k
        slot = ring(n, 2)
        for o in range(4):
            ostage(k, o).wait()
        if w == CW:
            obuf[ring(n, 4)] = _dot(seen[...], wob[slot])
        else:
            for r in halves:
                obuf[ring(n, 4), r, :w] = _dot(seen[r, :], wob[slot, :, :w])
        part_copy(k).start()

    @pl.loop(1, G)
    def _(g):
        @pl.when(g + 3 < G)
        def _():
            own_n(g + 3)

        got_f(g)
        pass_d(g, 3).start()
        stage(g, 6).start()
        stage(g, 4).start()
        got_d(g, 1)
        stage(g, 5).start()
        slot = lax.rem(g, 2)

        for b in range(4):
            stage(g, b).wait()
        for r, a in zip(halves, (y, A)):
            acc[r, :] = _dot(a[:, : 4 * ROWS], wbuf[slot, : 4 * ROWS, :])

        @pl.when(g + 1 < G)
        def _():
            relay_n(g + 1, 1)
            pass_d(g + 1, 1).start()

        @pl.when(g == G - 2)
        def _():
            wo_m(head[1]).start()

            @pl.loop(2, NC + 1)
            def _(n):
                wo_m(block(n)).start()

            for k in tail:
                wo_m(k).start()

        got_d(g, 3)
        stage(g, 7).start()
        stage(g, 4).wait()
        stage(g, 5).wait()
        for r, a in zip(halves, (y, A)):
            acc[r, :] += _dot(a[:, 4 * ROWS : 6 * ROWS], wbuf[slot, 4 * ROWS : 6 * ROWS, :])
        stage(g, 6).wait()
        stage(g, 7).wait()
        for r, a, to in zip(halves, (y, A), (own_rows, mate_rows)):
            t = acc[r, :] + _dot(a[:, 6 * ROWS :], wbuf[slot, 6 * ROWS :, :])
            q_s[to, :] = _turn(t.astype(jnp.bfloat16).astype(jnp.float32), cos[to, :], sin[to, :])

        @pl.when(g + 1 < G)
        def _():
            stage_early(g + 1)

        @pl.when(g == HEADS // 2)
        def _():
            share(head[0])

        @pl.when(g == G - 1)
        def _():
            fetch(head[0])

        attend(g)

    multiply(head[0])
    fetch(head[1])
    multiply(head[1])

    @pl.loop(2, NC + 1)
    def _(n):
        @pl.when(n >= 6)
        def _():
            part_copy(block(n - 4)).wait_send()

        for k in head:

            @pl.when(n == k[0] + 4)
            def _():
                part_copy(k).wait_send()

        fetch(block(n))
        multiply(block(n))

        @pl.when(n >= 4)
        def _():
            finish(block(n - 2))

        for k in head:

            @pl.when(n == k[0] + 2)
            def _():
                finish(k)

    late = [block(n) for n in range(NC - 3, NC + 1)] + tail
    for m in (4, 5):
        part_copy(late[m - 4]).wait_send()
        fetch(late[m])
        multiply(late[m])
        finish(late[m - 2])
    for m in (4, 5):
        finish(late[m])
    for m in (2, 3, 4, 5):
        part_copy(late[m]).wait_send()

    sent = WQ.at[:, rows(0), :]
    for k, dev in ((sn, nb), (sm, mb), (sf, mb), (sd.at[1], sib), (sd.at[2], sib), (sd.at[3], sib)):
        remote(sent, sent, k, rm.at[0], dev).wait_send()
    moved(0, 0, sd.at[0], rm.at[0], sib).wait_send()
    own_d().wait_send()
    wo_d().wait_send()
    sent = WO.at[:, rows(0), :]
    for k, dev in ((swm, mb), (swd, sib)):
        remote(sent, sent, k, rm.at[0], dev).wait_send()
    for p in range(PIECES):
        x_whole(p).wait_send()
    for k, dev in enumerate((nb, mb, sib, nb, sib, sib, sib)):
        for which in range(2):
            kv_block(0, 0, sk.at[k, which], dev).wait_send()


def solution(mesh):
    def step(x, gain, wq, wk, wv, wo):
        rate = THETA ** (-np.arange(HALF) / HALF)
        angle = np.concatenate([np.arange(OWN), OWN * np.arange(8)])[:, None] * rate
        turns = np.concatenate([np.cos(angle), np.sin(angle)], axis=1).astype(np.float32)
        bf16, f32, dma = jnp.bfloat16, jnp.float32, pltpu.SemaphoreType.DMA
        hbm, vmem = pl.BlockSpec(memory_space=pltpu.HBM), pl.BlockSpec(memory_space=pltpu.VMEM)
        out = pl.pallas_call(
            _kernel,
            out_shape=[
                pltpu.VMEM((OWN, D), bf16),
                jax.ShapeDtypeStruct((G, D, HEAD), bf16),
                jax.ShapeDtypeStruct((NC + 1, HEADS * HEAD, CW), bf16),
                jax.ShapeDtypeStruct((NC + 1, OWN, CW), f32),
                jax.ShapeDtypeStruct((ROWS, HEADS * HEAD), bf16),
                jax.ShapeDtypeStruct((ROWS, D), bf16),
            ],
            in_specs=[hbm, vmem, hbm, hbm, hbm, hbm, hbm],
            out_specs=[pl.BlockSpec(memory_space=pltpu.VMEM)] + [hbm] * 5,
            scratch_shapes=[
                pltpu.VMEM((OWN, D), bf16),
                pltpu.VMEM((2, 8 * OWN, HEAD), bf16),
                pltpu.VMEM((HEAD + 8, 8 * OWN), bf16),
                pltpu.VMEM((TOK, HEADS * HEAD), bf16),
                pltpu.VMEM((2, D, HEAD), bf16),
                pltpu.VMEM((TOK, HEAD), bf16),
                pltpu.VMEM((TOK, HEAD), f32),
                pltpu.VMEM((1, TOK), f32),
                pltpu.VMEM((HEAD + 8, TOK), f32),
                pltpu.VMEM((2, HEADS * HEAD, CW), bf16),
                pltpu.VMEM((4, TOK, CW), f32),
                pltpu.VMEM((2, OWN, CW), f32),
                pltpu.VMEM((2, OWN, CW // 2), f32),
                pltpu.VMEM((2, OWN, CW), bf16),
                pltpu.VMEM((OWN + 8, HEAD), f32),
                *[pltpu.VMEM((TOK, HALF), f32)] * 2,
                pltpu.VMEM((1, D), f32),
                *(dma, dma((G, 2)), dma, dma((G,)), dma, dma((G, 2))),
                *(dma((4,)), dma((G, 3)), dma((2,)), dma((3,))),
                *[dma((PIECES,))] * 3,
                dma((7, 2)),
                dma((2, 8)),
                dma((2, 8)),
                *(dma, dma((NC + 3,)), dma, dma((NC + 3,))),
                dma((2, 4)),
                *(dma((4,)), dma((NC + 3,))),
                *[dma((2,))] * 2,
                dma,
            ],
            compiler_params=pltpu.CompilerParams(collective_id=0, has_side_effects=True, vmem_limit_bytes=VMEM),
            cost_estimate=pl.CostEstimate(flops=2 * 10**11, bytes_accessed=4 * 10**8, transcendentals=5 * 10**7),
        )(x, gain, wk, wv, wq, wo, jnp.asarray(turns))
        return out[0]

    tokens, whole = P(("dp", "sp"), None), P("sp", None)
    return jax.shard_map(
        step,
        mesh=mesh,
        in_specs=(tokens, P(None), whole, whole, whole, whole),
        out_specs=tokens,
        check_vma=False,
    )
```
